32 devices in a mesh: samp: 16 (over z, y, x), feat: 2 (over core).
Axes of the slice: x: 2, y: 2, z: 4, core: 2. Of those that a mesh axis runs over, the one named last changes fastest.
Arguments:
- design_matrix: bfloat16 [2048, 32768], P('samp', 'feat'), may hold values from -0.046875 to 0.046875
- labels: int32 [2048], P('samp'), may hold values from 0 to 1
- weights: float32 [16, 32768], P(None, ('feat', 'samp')), may hold values from -6 to 6
- lambdas: float32 [16], replicated, may hold values from 0.05 to 1
- sketch: bfloat16 [32768, 384], P(('feat', 'samp')), may hold values from -0.03125 to 0.03125
- sketch_values: float32 [384], replicated, may hold values from 0.05 to 2
Outputs:
- new_weights: float32 [16, 32768], P(None, ('feat', 'samp'))
The draws below stay inside these ranges and needn't reach their ends.
All inputs are finite; a program needn't handle non-finite values.
Results may differ from the reference program's by a relative error of at most 0.004.
Values may be sent and summed in bfloat16 or wider, within the bound.
No kernel may reach another device: no remote copies, remote signals or barrier semaphores. Data moves between devices by JAX's collectives and lax.ppermute only.
A program may use at most 64 MiB of HBM per device.

```python
import math
import jax
import jax.numpy as jnp
from jax import lax

FEATURES = 32768
RANK = 384
STRENGTHS = 16
ITERS = 2
SAMPLES = 2048


def place_ends(result, key, low, largest):
    shape = result.shape
    index_at = [jax.random.randint(jax.random.fold_in(key, axis), (), 0, shape[axis]) for axis in range(len(shape))]
    result = result.at[tuple(index_at)].set(low)
    longest = shape.index(max(shape))
    index_at[longest] = (index_at[longest] + 1) % shape[longest]
    return result.at[tuple(index_at)].set(largest)


def strengthened(array, own_key, source, target, blocks, factor):
    owner, partner = [(jnp.arange(array.shape[position]) // (array.shape[position] // blocks)).reshape([-1 if axis == position else 1 for axis in range(array.ndim)]) for position in (source, target)]
    chosen = jax.random.permutation(own_key, blocks)[partner]
    strong = (owner == chosen) | (owner == (partner + blocks // 2) % blocks)
    return jnp.where(strong, factor * array, array)


def shard_levels(own_key, shape, pieces, low, top_value):
    gain, own = 1.0, jax.random.fold_in(own_key, 6)
    for position, shards_of in pieces:
        steps = jnp.exp(jax.random.uniform(jax.random.fold_in(own, position), (shards_of,), jnp.float32, low / len(pieces), top_value / len(pieces)))
        gain = gain * jnp.repeat(steps, shape[position] // shards_of).reshape([-1 if axis == position else 1 for axis in range(len(shape))])
    return gain


def noise(stream_key, extent, width, most, split=(), held_as=jnp.bfloat16):
    gain = shard_levels(stream_key, extent, split, -0.22, 0.18) if split else 1.0
    values = jax.random.normal(stream_key, extent, jnp.float32) * width * gain
    return jnp.minimum(jnp.maximum(values, -most), most).astype(held_as)


def heavy_noise(key, shape, scale, bound, shards, heavy, kind=jnp.bfloat16):
    values = scale * jax.random.normal(key, shape, jnp.float32)
    if shards:
        values = values * shard_levels(key, shape, shards, -0.22, 0.18)
    return jnp.clip(strengthened(values, jax.random.fold_in(key, 3), *heavy), -bound, bound).astype(kind)


def setup_inputs(seed: int = 0) -> dict:
    arg_keys = jax.random.split(jax.random.key(seed), 7)
    design_matrix = heavy_noise(arg_keys[0], (SAMPLES, FEATURES), FEATURES ** -0.5, 0.046875, ((0, 16), (1, 2)), (0, 1, 16, 2.0))
    labels = place_ends(jax.random.randint(arg_keys[1], (SAMPLES,), 0, 2), jax.random.fold_in(arg_keys[1], 1), 0, 1).astype(jnp.int32)
    weights = noise(arg_keys[2], (STRENGTHS, FEATURES), 1.0, 6.0, ((1, 32),), jnp.float32)
    lambdas = jnp.clip(jnp.exp(jax.random.uniform(arg_keys[3], (STRENGTHS,), jnp.float32, math.log(0.05), math.log(1.0))), 0.05, 1.0)
    sketch = noise(arg_keys[4], (FEATURES, RANK), FEATURES ** -0.5, 0.03125, ((0, 32),))
    sketch_values = jnp.clip(jnp.exp(jax.random.uniform(arg_keys[5], (RANK,), jnp.float32, math.log(0.05), math.log(2.0))), 0.05, 2.0)
    return dict(design_matrix=design_matrix, labels=labels, weights=weights, lambdas=lambdas, sketch=sketch, sketch_values=sketch_values)


def reference(design_matrix, labels, weights, lambdas, sketch, sketch_values):
    sketch_full = sketch.astype(jnp.float32)
    smallest = jnp.min(sketch_values)
    ratios = (smallest + lambdas[:, None]) / (sketch_values[None, :] + lambdas[:, None]) - 1.0

    def apply_rows(vector):
        return lax.dot_general(vector.astype(jnp.bfloat16), design_matrix, (((1,), (1,)), ((), ())), preferred_element_type=jnp.float32)

    def apply_columns(values):
        return jnp.dot(values, design_matrix, preferred_element_type=jnp.float32)

    def precondition(residual):
        projected = jnp.dot(residual, sketch_full, precision=lax.Precision.HIGHEST)
        correction = lax.dot_general(ratios * projected, sketch_full, (((1,), (1,)), ((), ())), precision=lax.Precision.HIGHEST)
        precond_res = residual + correction
        return precond_res, jnp.sum(residual * precond_res, axis=1)

    logits = apply_rows(weights)
    probability = jax.nn.sigmoid(logits)
    hessian_diag = probability * (1.0 - probability)
    miss_rows = (probability - labels[None, :].astype(jnp.float32)).astype(jnp.bfloat16)
    gradient = apply_columns(miss_rows) + lambdas[:, None] * weights
    residual = -gradient
    precond_res, res_dot = precondition(residual)
    direction = precond_res
    update = jnp.zeros_like(weights)
    for iteration in range(ITERS):
        image_rows = apply_rows(direction)
        hess_dir = apply_columns((hessian_diag * image_rows).astype(jnp.bfloat16)) + lambdas[:, None] * direction
        step_size = res_dot / jnp.sum(direction * hess_dir, axis=1)
        update = update + step_size[:, None] * direction
        if iteration + 1 < ITERS:
            residual = residual - step_size[:, None] * hess_dir
            precond_res, new_dot = precondition(residual)
            direction = precond_res + (new_dot / res_dot)[:, None] * direction
            res_dot = new_dot
    return weights + update
```

```python
import jax
import jax.numpy as jnp
from jax import lax
from jax.sharding import PartitionSpec as P

ITERS = 2
LANES = 128


def pack(values):
    high = lax.reduce_precision(values, 8, 7)
    rest = values - high
    middle = lax.reduce_precision(rest, 8, 7)
    low = rest - middle
    parts = jnp.stack([high, middle, low], axis=1)
    return jnp.pad(parts, ((0, 0), (0, LANES - 3))).astype(jnp.bfloat16)


def unpack(summed):
    return summed[:, 0] + summed[:, 1] + summed[:, 2]


def make_shards(samp, feat):
    def exchange(blocks):
        return lax.all_to_all(blocks, "samp", 0, 0)

    def gather(block):
        return exchange(jnp.broadcast_to(block[None], (samp,) + block.shape))

    def feat_sum(values):
        if feat == 2:
            return values + lax.ppermute(values, "feat", [(0, 1), (1, 0)])
        return lax.psum(values, "feat")

    def shards(design_matrix, labels, weights, lambdas, sketch, sketch_values):
        strengths, width = weights.shape
        samples, block = design_matrix.shape
        rank = sketch.shape[1]
        sketch_full = sketch.astype(jnp.float32)
        smallest = jnp.min(sketch_values)
        lam = lambdas[:, None]
        ratios = (smallest + lam) / (sketch_values[None, :] + lam) - 1.0

        def apply_rows(vector):
            whole = gather(vector.astype(jnp.bfloat16))
            flat = whole.transpose(1, 0, 2).reshape(strengths, block)
            partial_rows = lax.dot_general(
                flat, design_matrix, (((1,), (1,)), ((), ())), preferred_element_type=jnp.float32
            )
            squares = jnp.sum(jnp.square(flat.astype(jnp.float32)), axis=1)
            both = jnp.concatenate(
                [partial_rows, jnp.broadcast_to(squares[:, None], (strengths, LANES))], axis=1
            )
            both = feat_sum(both)
            return both[:, :samples], both[:, samples]

        def apply_columns(values, scalars):
            partial = lax.dot_general(
                values, design_matrix, (((1,), (0,)), ((), ())), preferred_element_type=jnp.float32
            )
            blocks = partial.astype(jnp.bfloat16).reshape(strengths, samp, width).transpose(1, 0, 2)
            if scalars is not None:
                extra = jnp.broadcast_to(pack(scalars)[None], (samp, strengths, LANES))
                blocks = jnp.concatenate([blocks, extra], axis=2)
            summed = jnp.sum(exchange(blocks).astype(jnp.float32), axis=0)
            if scalars is None:
                return summed, None
            return summed[:, :width], unpack(summed[:, width:])

        def precondition(residual):
            projected = jnp.dot(residual, sketch_full, precision=lax.Precision.HIGHEST)
            square = jnp.sum(residual * residual, axis=1)
            payload = jnp.concatenate([projected.astype(jnp.bfloat16), pack(square)], axis=1)
            summed = feat_sum(jnp.sum(gather(payload).astype(jnp.float32), axis=0))
            projected = summed[:, :rank]
            scaled = ratios * projected
            correction = lax.dot_general(
                scaled, sketch_full, (((1,), (1,)), ((), ())), precision=lax.Precision.HIGHEST
            )
            res_dot = unpack(summed[:, rank:]) + jnp.sum(scaled * projected, axis=1)
            return residual + correction, res_dot

        logits, _ = apply_rows(weights)
        probability = jax.nn.sigmoid(logits)
        hessian_diag = probability * (1.0 - probability)
        miss_rows = (probability - labels[None, :].astype(jnp.float32)).astype(jnp.bfloat16)
        residual = -(apply_columns(miss_rows, None)[0] + lam * weights)
        precond_res, res_dot = precondition(residual)
        direction = precond_res
        update = jnp.zeros_like(residual)
        for iteration in range(ITERS):
            image_rows, square = apply_rows(direction)
            image = (hessian_diag * image_rows).astype(jnp.bfloat16)
            energy = jnp.sum(image.astype(jnp.float32) * image_rows, axis=1)
            if iteration + 1 < ITERS:
                columns, energy = apply_columns(image, energy)
                step_size = res_dot / (energy + lambdas * square)
                update = update + step_size[:, None] * direction
                residual = residual - step_size[:, None] * (columns + lam * direction)
                precond_res, new_dot = precondition(residual)
                direction = precond_res + (new_dot / res_dot)[:, None] * direction
                res_dot = new_dot
            else:
                total = gather(jnp.broadcast_to(energy[:, None], (strengths, LANES)))
                energy = jnp.sum(total, axis=0)[:, 0]
                step_size = res_dot / (energy + lambdas * square)
                update = update + step_size[:, None] * direction
        return weights + update

    return shards


def solution(mesh):
    return jax.shard_map(
        make_shards(mesh.shape["samp"], mesh.shape["feat"]),
        mesh=mesh,
        in_specs=(
            P("samp", "feat"),
            P("samp"),
            P(None, ("feat", "samp")),
            P(),
            P(("feat", "samp"), None),
            P(),
        ),
        out_specs=P(None, ("feat", "samp")),
        check_vma=False,
    )
```

```python
import math

import jax
import jax.numpy as jnp
from jax import lax
from jax.experimental import pallas as pl
from jax.experimental.pallas import tpu as pltpu
from jax.sharding import PartitionSpec as P

ITERS = 2
LANES = 128
SUBLANES = 8
LARGEST = 0.09375
HALF_RANGE = 60000.0


def split(values):
    high = values.astype(jnp.bfloat16)
    rest = values - high.astype(jnp.float32)
    middle = rest.astype(jnp.bfloat16)
    low = (rest - middle.astype(jnp.float32)).astype(jnp.bfloat16)
    return high, middle, low


def exact_dot(values, other, contract):
    rows = values.shape[0]
    product = lax.dot_general(
        jnp.concatenate(split(values), axis=0),
        other,
        (((1,), (contract,)), ((), ())),
        preferred_element_type=jnp.float32,
    )
    return product[:rows] + product[rows : 2 * rows] + product[2 * rows :]


def pack(column):
    high, middle, low = (part.astype(jnp.float32) for part in split(column))
    lane = lax.broadcasted_iota(jnp.int32, (column.shape[0], LANES), 1)
    zero = jnp.zeros((column.shape[0], LANES), jnp.float32)
    tile = jnp.where(lane == 0, high, jnp.where(lane == 1, middle, jnp.where(lane == 2, low, zero)))
    return tile.astype(jnp.bfloat16)


def wide(column):
    return jnp.broadcast_to(column, (column.shape[0], LANES))


def repeat(out_ref, block):
    for part in range(out_ref.shape[0]):
        out_ref[part] = block


def start_body(weights_ref, lam_ref, payload_ref, lam_out):
    repeat(payload_ref, weights_ref[...].astype(jnp.bfloat16))
    lam_out[...] = lam_ref[...]


def rows_body(whole_ref, design_ref, out_ref, kept_ref):
    del kept_ref
    parts, strengths, width = whole_ref.shape
    samples = design_ref.shape[0]
    total = jnp.zeros((strengths, samples), jnp.float32)
    squares = jnp.zeros((strengths, width), jnp.float32)
    for part in range(parts):
        block = whole_ref[part]
        total += lax.dot_general(
            block,
            design_ref[:, part * width : (part + 1) * width],
            (((1,), (1,)), ((), ())),
            preferred_element_type=jnp.float32,
        )
        values = block.astype(jnp.float32)
        squares += values * values
    out_ref[:, :samples] = total
    out_ref[:, samples:] = wide(jnp.sum(squares, axis=1, keepdims=True))


def columns(values, design_ref, out_ref, scale=None):
    width = design_ref.shape[1] // out_ref.shape[0]
    for part in range(out_ref.shape[0]):
        block = lax.dot_general(
            values,
            design_ref[:, part * width : (part + 1) * width],
            (((1,), (0,)), ((), ())),
            preferred_element_type=jnp.float32,
        )
        if scale is not None:
            block = block * scale
        out_ref[part, :, :width] = block.astype(out_ref.dtype)


def miss_body(scale, both_ref, other_ref, labels_ref, design_ref, hessian_ref, out_ref):
    samples = design_ref.shape[0]
    logits = both_ref[:, :samples] + other_ref[:, :samples]
    probability = 1.0 / (1.0 + jnp.exp(-logits))
    hessian_ref[...] = probability * (1.0 - probability)
    miss_rows = (probability - labels_ref[...].astype(jnp.float32)).astype(jnp.bfloat16)
    columns(miss_rows, design_ref, out_ref, scale)


def project(residual, sketch_ref, payload_ref):
    rank = sketch_ref.shape[1]
    projected = exact_dot(residual, sketch_ref[...], 0).astype(jnp.bfloat16)
    square = pack(jnp.sum(residual * residual, axis=1, keepdims=True))
    for part in range(payload_ref.shape[0]):
        payload_ref[part, :, :rank] = projected
        payload_ref[part, :, rank:] = square


def gradient_body(summed_ref, weights_ref, lam_ref, sketch_ref, residual_ref, payload_ref):
    residual = -(summed_ref[...] + lam_ref[:, :1] * weights_ref[...])
    residual_ref[...] = residual
    project(residual, sketch_ref, payload_ref)


def correct(summed_ref, other_ref, lam_ref, values_ref, sketch_ref, residual):
    rank = sketch_ref.shape[1]
    lam = lam_ref[:, :1]
    values = values_ref[...]
    smallest = jnp.min(values, axis=1, keepdims=True)
    ratios = (smallest + lam) / (values + lam) - 1.0
    summed = summed_ref[...] + other_ref[...]
    projected = summed[:, :rank]
    scaled = ratios * projected
    res_dot = jnp.sum(summed[:, rank:], axis=1, keepdims=True)
    res_dot = res_dot + jnp.sum(scaled * projected, axis=1, keepdims=True)
    return residual + exact_dot(scaled, sketch_ref[...], 1), res_dot


def first_body(
    summed_ref, other_ref, lam_ref, values_ref, sketch_ref, residual_ref,
    direction_ref, dot_ref, payload_ref,
):
    direction, res_dot = correct(
        summed_ref, other_ref, lam_ref, values_ref, sketch_ref, residual_ref[...]
    )
    direction_ref[...] = direction
    dot_ref[...] = wide(res_dot)
    repeat(payload_ref, direction.astype(jnp.bfloat16))


def next_body(
    summed_ref, other_ref, lam_ref, values_ref, sketch_ref, residual_ref, old_ref, old_dot_ref,
    direction_ref, dot_ref, payload_ref,
):
    precond_res, res_dot = correct(
        summed_ref, other_ref, lam_ref, values_ref, sketch_ref, residual_ref[...]
    )
    direction = precond_res + (res_dot / old_dot_ref[:, :1]) * old_ref[...]
    direction_ref[...] = direction
    dot_ref[...] = wide(res_dot)
    repeat(payload_ref, direction.astype(jnp.bfloat16))


def image_of(both_ref, other_ref, hessian_ref, square_ref):
    samples = hessian_ref.shape[1]
    both = both_ref[...] + other_ref[...]
    square_ref[...] = both[:, samples:]
    image_rows = both[:, :samples]
    image = (hessian_ref[...] * image_rows).astype(jnp.bfloat16)
    energy = jnp.sum(image.astype(jnp.float32) * image_rows, axis=1, keepdims=True)
    return image, energy


def image_body(both_ref, other_ref, hessian_ref, design_ref, square_ref, out_ref):
    image, energy = image_of(both_ref, other_ref, hessian_ref, square_ref)
    width = out_ref.shape[2] - LANES
    packed = pack(energy)
    for part in range(out_ref.shape[0]):
        out_ref[part, :, width:] = packed
    columns(image, design_ref, out_ref)


def step_body(
    received_ref, square_ref, dot_ref, lam_ref, direction_ref, residual_ref, update_ref, sketch_ref,
    new_residual_ref, new_update_ref, payload_ref,
):
    width = direction_ref.shape[1]
    summed = received_ref[0].astype(jnp.float32)
    for part in range(1, received_ref.shape[0]):
        summed += received_ref[part].astype(jnp.float32)
    lam = lam_ref[:, :1]
    energy = jnp.sum(summed[:, width:], axis=1, keepdims=True)
    step_size = dot_ref[:, :1] / (energy + lam * square_ref[:, :1])
    direction = direction_ref[...]
    new_update_ref[...] = update_ref[...] + step_size * direction
    residual = residual_ref[...] - step_size * (summed[:, :width] + lam * direction)
    new_residual_ref[...] = residual
    project(residual, sketch_ref, payload_ref)


def energy_body(both_ref, other_ref, hessian_ref, square_ref, payload_ref):
    _, energy = image_of(both_ref, other_ref, hessian_ref, square_ref)
    lane = lax.broadcasted_iota(jnp.int32, (SUBLANES, LANES), 1)
    tile = jnp.zeros((SUBLANES, LANES), jnp.float32)
    for group in range(energy.shape[0] // SUBLANES):
        tile = jnp.where(lane == group, energy[group * SUBLANES : (group + 1) * SUBLANES], tile)
    repeat(payload_ref, tile)


def finish_body(received_ref, square_ref, dot_ref, lam_ref, direction_ref, update_ref, out_ref):
    tile = received_ref[0]
    for part in range(1, received_ref.shape[0]):
        tile += received_ref[part]
    groups = direction_ref.shape[0] // SUBLANES
    energy = jnp.concatenate([tile[:, group : group + 1] for group in range(groups)], axis=0)
    step_size = dot_ref[:, :1] / (energy + lam_ref[:, :1] * square_ref[:, :1])
    out_ref[...] = update_ref[...] + step_size * direction_ref[...]


VMEM = pl.BlockSpec(memory_space=pltpu.VMEM)


def call(body, name, shapes, *operands, aliases={}):
    return pl.pallas_call(
        body,
        out_shape=[jax.ShapeDtypeStruct(shape, dtype) for shape, dtype in shapes],
        in_specs=[VMEM] * len(operands),
        out_specs=[VMEM] * len(shapes),
        input_output_aliases=aliases,
        compiler_params=pltpu.CompilerParams(vmem_limit_bytes=8 << 20),
        name=name,
    )(*operands)


def make_shards(samp, feat):
    def exchange(blocks):
        return lax.all_to_all(blocks, "samp", 0, 0)

    def feat_parts(values):
        if feat == 2:
            return values, lax.ppermute(values, "feat", [(0, 1), (1, 0)])
        return lax.psum(values, "feat"), jnp.zeros_like(values)

    def shards(design_matrix, labels, weights, lambdas, sketch, sketch_values):
        strengths, width = weights.shape
        samples = design_matrix.shape[0]
        rank = sketch.shape[1]
        single, half = jnp.float32, jnp.bfloat16
        field = ((strengths, width), single)
        scalars = ((strengths, LANES), single)
        spread = ((samp, strengths, width), half)
        payload = ((samp, strengths, rank + LANES), half)
        scale = 2.0 ** math.floor(math.log2(HALF_RANGE / (samples * LARGEST)))
        lam = jnp.broadcast_to(lambdas[:, None], (strengths, LANES))
        labels = labels[None, :]
        values = sketch_values[None, :]

        def apply_rows(blocks, design):
            both, design = call(
                rows_body, "rows",
                [((strengths, samples + LANES), single), (design.shape, design.dtype)],
                exchange(blocks), design, aliases={1: 1},
            )
            return feat_parts(both), design

        def reduced(blocks):
            return feat_parts(jnp.sum(exchange(blocks).astype(single), axis=0))

        blocks, lam = call(start_body, "start", [spread, scalars], weights, lam)
        parts, design = apply_rows(blocks, design_matrix)
        hessian_diag, blocks = call(
            lambda *refs: miss_body(scale, *refs),
            "miss",
            [((strengths, samples), single), ((samp, strengths, width), single)],
            *parts, labels, design,
        )
        summed = jnp.sum(exchange(blocks.astype(jnp.float16)).astype(single), axis=0) * (1.0 / scale)
        residual, blocks = call(
            gradient_body, "gradient", [field, payload], summed, weights, lam, sketch
        )
        direction, res_dot, blocks = call(
            first_body, "first", [field, scalars, spread], *reduced(blocks), lam, values, sketch, residual
        )
        update = weights
        for iteration in range(ITERS):
            parts, design = apply_rows(blocks, design)
            if iteration + 1 == ITERS:
                tiny = ((samp, SUBLANES, LANES), single)
                square, blocks = call(energy_body, "energy", [scalars, tiny], *parts, hessian_diag)
                return call(
                    finish_body, "finish", [field],
                    exchange(blocks), square, res_dot, lam, direction, update,
                )[0]
            square, blocks = call(
                image_body, "image", [scalars, ((samp, strengths, width + LANES), half)],
                *parts, hessian_diag, design,
            )
            residual, update, blocks = call(
                step_body, "step", [field, field, payload],
                exchange(blocks), square, res_dot, lam, direction, residual, update, sketch,
            )
            direction, res_dot, blocks = call(
                next_body, "next", [field, scalars, spread],
                *reduced(blocks), lam, values, sketch, residual, direction, res_dot,
            )

    return shards


def solution(mesh):
    return jax.shard_map(
        make_shards(mesh.shape["samp"], mesh.shape["feat"]),
        mesh=mesh,
        in_specs=(
            P("samp", "feat"),
            P("samp"),
            P(None, ("feat", "samp")),
            P(),
            P(("feat", "samp"), None),
            P(),
        ),
        out_specs=P(None, ("feat", "samp")),
        check_vma=False,
    )
```

```python
import math

import jax
import jax.numpy as jnp
from jax import lax
from jax.experimental import pallas as pl
from jax.experimental.pallas import tpu as pltpu
from jax.sharding import PartitionSpec as P

ITERS = 2
LANES = 128
SUBLANES = 8
LARGEST = 0.09375
HALF_RANGE = 60000.0


def split(values):
    high = values.astype(jnp.bfloat16)
    rest = values - high.astype(jnp.float32)
    middle = rest.astype(jnp.bfloat16)
    low = (rest - middle.astype(jnp.float32)).astype(jnp.bfloat16)
    return high, middle, low


def exact_dot(values, other, contract):
    rows = values.shape[0]
    product = lax.dot_general(
        jnp.concatenate(split(values), axis=0),
        other,
        (((1,), (contract,)), ((), ())),
        preferred_element_type=jnp.float32,
    )
    return product[:rows] + product[rows : 2 * rows] + product[2 * rows :]


def pack(*columns_in):
    rows = columns_in[0].shape[0]
    lane = lax.broadcasted_iota(jnp.int32, (rows, LANES), 1)
    tile = jnp.zeros((rows, LANES), jnp.float32)
    for place, column in enumerate(columns_in):
        for index, part in enumerate(split(column)):
            tile = jnp.where(lane == 3 * place + index, part.astype(jnp.float32), tile)
    return tile


def unpack(tile, place):
    return jnp.sum(tile[:, 3 * place : 3 * place + 3], axis=1, keepdims=True)


def wide(column):
    return jnp.broadcast_to(column, (column.shape[0], LANES))


def repeat(out_ref, block):
    for part in range(out_ref.shape[0]):
        out_ref[part] = block


def load_body(offsets_ref, design_ref, out_ref, sems):
    parts = offsets_ref.shape[0]
    width = design_ref.shape[1] // parts
    copies = []
    for part in range(parts):
        offset = pl.multiple_of(offsets_ref[part], width)
        copies.append(
            pltpu.make_async_copy(
                design_ref.at[:, pl.ds(offset, width)],
                out_ref.at[:, pl.ds(part * width, width)],
                sems.at[part],
            )
        )
    for copy in copies:
        copy.start()
    for copy in copies:
        copy.wait()


def rows_body(*refs):
    *whole_refs, design_ref, extra_ref, out_ref = refs
    rows, strengths, width = whole_refs[0].shape
    samples = design_ref.shape[0]
    total = jnp.zeros((strengths, samples), jnp.float32)
    squares = jnp.zeros((strengths, width), jnp.float32)
    part = 0
    for whole_ref in whole_refs:
        for row in range(rows):
            block = whole_ref[row]
            total += lax.dot_general(
                block,
                design_ref[:, part * width : (part + 1) * width],
                (((1,), (1,)), ((), ())),
                preferred_element_type=jnp.float32,
            )
            values = block.astype(jnp.float32)
            squares += values * values
            part += 1
    out_ref[:, :samples] = total
    lane = lax.broadcasted_iota(jnp.int32, (strengths, LANES), 1)
    square = jnp.sum(squares, axis=1, keepdims=True)
    out_ref[:, samples:] = jnp.where(lane == 0, square, extra_ref[...])


def columns(values, design_ref, out_refs, scale=None):
    rows = out_refs[0].shape[0]
    width = design_ref.shape[1] // (rows * len(out_refs))
    part = 0
    for out_ref in out_refs:
        for row in range(rows):
            block = lax.dot_general(
                values,
                design_ref[:, part * width : (part + 1) * width],
                (((1,), (0,)), ((), ())),
                preferred_element_type=jnp.float32,
            )
            if scale is not None:
                block = block * scale
            out_ref[row, :, :width] = block.astype(out_ref.dtype)
            part += 1


def miss_body(scale, both_ref, other_ref, labels_ref, design_ref, hessian_ref, *out_refs):
    samples = design_ref.shape[0]
    logits = both_ref[:, :samples] + other_ref[:, :samples]
    probability = 1.0 / (1.0 + jnp.exp(-logits))
    hessian_ref[...] = probability * (1.0 - probability)
    miss_rows = (probability - labels_ref[...].astype(jnp.float32)).astype(jnp.bfloat16)
    columns(miss_rows, design_ref, out_refs, scale)


def square_of(residual):
    return jnp.sum(residual * residual, axis=1, keepdims=True)


def gradient_body(summed_ref, weights_ref, lam_ref, sketch_ref, residual_ref, square_ref, payload_ref):
    residual = -(summed_ref[...] + lam_ref[:, :1] * weights_ref[...])
    residual_ref[...] = residual
    lane = lax.broadcasted_iota(jnp.int32, square_ref.shape, 1)
    square_ref[...] = jnp.where(lane == 1, square_of(residual), 0.0)
    repeat(payload_ref, exact_dot(residual, sketch_ref[...], 0).astype(jnp.bfloat16))


def correct(summed_ref, other_ref, lam_ref, values_ref, sketch_ref):
    rank = sketch_ref.shape[1]
    lam = lam_ref[:, :1]
    values = values_ref[...]
    smallest = jnp.min(values, axis=1, keepdims=True)
    ratios = (smallest + lam) / (values + lam) - 1.0
    projected = summed_ref[:, :rank] + other_ref[:, :rank]
    scaled = ratios * projected
    return exact_dot(scaled, sketch_ref[...], 1), jnp.sum(scaled * projected, axis=1, keepdims=True)


def first_body(
    summed_ref, other_ref, lam_ref, values_ref, sketch_ref, residual_ref,
    direction_ref, part_ref, half_ref,
):
    correction, part = correct(summed_ref, other_ref, lam_ref, values_ref, sketch_ref)
    direction = residual_ref[...] + correction
    direction_ref[...] = direction
    part_ref[...] = wide(part)
    half_ref[...] = direction.astype(jnp.bfloat16)


def next_body(
    summed_ref, other_ref, lam_ref, values_ref, sketch_ref, residual_ref, old_ref, old_dot_ref,
    direction_ref, dot_ref, half_ref,
):
    rank = sketch_ref.shape[1]
    correction, part = correct(summed_ref, other_ref, lam_ref, values_ref, sketch_ref)
    res_dot = part + unpack(summed_ref[:, rank:] + other_ref[:, rank:], 0)
    precond_res = residual_ref[...] + correction
    direction = precond_res + (res_dot / old_dot_ref[:, :1]) * old_ref[...]
    direction_ref[...] = direction
    dot_ref[...] = wide(res_dot)
    half_ref[...] = direction.astype(jnp.bfloat16)


def image_of(both_ref, other_ref, hessian_ref, square_ref):
    samples = hessian_ref.shape[1]
    both = both_ref[...] + other_ref[...]
    square_ref[...] = both[:, samples:]
    image_rows = both[:, :samples]
    image = (hessian_ref[...] * image_rows).astype(jnp.bfloat16)
    energy = jnp.sum(image.astype(jnp.float32) * image_rows, axis=1, keepdims=True)
    return image, energy, both[:, samples + 1 : samples + 2]


def image_body(both_ref, other_ref, hessian_ref, design_ref, square_ref, *out_refs):
    image, energy, residual_square = image_of(both_ref, other_ref, hessian_ref, square_ref)
    width = out_refs[0].shape[2] - LANES
    packed = pack(energy, residual_square)
    for out_ref in out_refs:
        for row in range(out_ref.shape[0]):
            out_ref[row, :, width:] = packed.astype(out_ref.dtype)
    columns(image, design_ref, out_refs)


def fold_body(near, *refs):
    own_ref, *received_refs = refs[:near]
    kept_ref, *sent_refs = refs[near:]
    for row in range(own_ref.shape[0]):
        total = own_ref[row]
        for received_ref in received_refs:
            total += received_ref[row].astype(jnp.float32)
        width = total.shape[1] - LANES
        tile = total[:, width:]
        target_ref = ([kept_ref] + sent_refs)[row]
        packed = pack(unpack(tile, 0), unpack(tile, 1))
        target_ref[:, :width] = total[:, :width].astype(target_ref.dtype)
        target_ref[:, width:] = packed.astype(target_ref.dtype)


def step_body(far, *refs):
    kept_ref, *received_refs = refs[:far]
    (
        square_ref, part_ref, lam_ref, direction_ref, residual_ref, update_ref, sketch_ref,
        new_residual_ref, new_update_ref, dot_ref, payload_ref,
    ) = refs[far:]
    width = direction_ref.shape[1]
    rank = sketch_ref.shape[1]
    summed = kept_ref[...]
    for received_ref in received_refs:
        summed += received_ref[...].astype(jnp.float32)
    tile = summed[:, width:]
    lam = lam_ref[:, :1]
    res_dot = part_ref[:, :1] + unpack(tile, 1)
    dot_ref[...] = wide(res_dot)
    step_size = res_dot / (unpack(tile, 0) + lam * square_ref[:, :1])
    direction = direction_ref[...]
    new_update_ref[...] = update_ref[...] + step_size * direction
    residual = residual_ref[...] - step_size * (summed[:, :width] + lam * direction)
    new_residual_ref[...] = residual
    projected = exact_dot(residual, sketch_ref[...], 0).astype(jnp.bfloat16)
    packed = pack(square_of(residual)).astype(jnp.bfloat16)
    for part in range(payload_ref.shape[0]):
        payload_ref[part, :, :rank] = projected
        payload_ref[part, :, rank:] = packed


def energy_body(both_ref, other_ref, hessian_ref, square_ref, payload_ref):
    _, energy, _ = image_of(both_ref, other_ref, hessian_ref, square_ref)
    lane = lax.broadcasted_iota(jnp.int32, (SUBLANES, LANES), 1)
    tile = jnp.zeros((SUBLANES, LANES), jnp.float32)
    for group in range(energy.shape[0] // SUBLANES):
        tile = jnp.where(lane == group, energy[group * SUBLANES : (group + 1) * SUBLANES], tile)
    repeat(payload_ref, tile)


def finish_body(received_ref, square_ref, dot_ref, lam_ref, direction_ref, update_ref, out_ref):
    tile = received_ref[0]
    for part in range(1, received_ref.shape[0]):
        tile += received_ref[part]
    groups = direction_ref.shape[0] // SUBLANES
    energy = jnp.concatenate([tile[:, group : group + 1] for group in range(groups)], axis=0)
    step_size = dot_ref[:, :1] / (energy + lam_ref[:, :1] * square_ref[:, :1])
    out_ref[...] = update_ref[...] + step_size * direction_ref[...]


VMEM = pl.BlockSpec(memory_space=pltpu.VMEM)


def call(body, name, shapes, *operands):
    return pl.pallas_call(
        body,
        out_shape=[jax.ShapeDtypeStruct(shape, dtype) for shape, dtype in shapes],
        in_specs=[VMEM] * len(operands),
        out_specs=[VMEM] * len(shapes),
        compiler_params=pltpu.CompilerParams(vmem_limit_bytes=8 << 20),
        name=name,
    )(*operands)


def load(design, offsets):
    return pl.pallas_call(
        load_body,
        out_shape=pltpu.VMEM(design.shape, design.dtype),
        in_specs=[pl.BlockSpec(memory_space=pltpu.SMEM), pl.BlockSpec(memory_space=pltpu.HBM)],
        out_specs=VMEM,
        scratch_shapes=[pltpu.SemaphoreType.DMA((offsets.shape[0],))],
        compiler_params=pltpu.CompilerParams(vmem_limit_bytes=1 << 20),
        name="load",
    )(offsets, design)


def make_shards(samp, feat):
    near = min(samp, 4)
    far = samp // near

    def swap(values, distance):
        return lax.ppermute(values, "samp", [(i, i ^ distance) for i in range(samp)])

    def far_order():
        return sorted(range(1, far), key=lambda k: (k + 1) % far)

    def swap_far(values_of):
        return {k: swap(values_of(k), near * k) for k in far_order()}

    def gather(block):
        received = swap_far(lambda k: block)
        column = jnp.stack([block] + [received[k] for k in range(1, far)])
        plane = {j: swap(column, j) for j in reversed(range(1, near))}
        return [column] + [plane[j] for j in range(1, near)]

    def exchange(blocks):
        return lax.all_to_all(blocks, "samp", 0, 0)

    def feat_parts(values):
        if feat == 2:
            return values, lax.ppermute(values, "feat", [(0, 1), (1, 0)])
        return lax.psum(values, "feat"), jnp.zeros_like(values)

    def shards(design_matrix, labels, weights, lambdas, sketch, sketch_values):
        strengths, width = weights.shape
        samples = design_matrix.shape[0]
        rank = sketch.shape[1]
        single, half = jnp.float32, jnp.bfloat16
        field = ((strengths, width), single)
        scalars = ((strengths, LANES), single)
        spread = ((strengths, width), half)
        scale = 2.0 ** math.floor(math.log2(HALF_RANGE / (samples * near * LARGEST)))
        lam = jnp.broadcast_to(lambdas[:, None], (strengths, LANES))
        labels = labels[None, :]
        values = sketch_values[None, :]
        mine = lax.axis_index("samp")
        places = jnp.array([k * near + j for j in range(near) for k in range(far)], jnp.int32)
        places = jnp.bitwise_xor(mine, places)
        if width % LANES == 0:
            design = load(design_matrix, places * width)
        else:
            design = design_matrix.reshape(samples, samp, width)
            design = jnp.take(design, places, axis=1).reshape(design_matrix.shape)

        def apply_rows(block, extra):
            shape = ((strengths, samples + LANES), single)
            return feat_parts(call(rows_body, "rows", [shape], *gather(block), design, extra)[0])

        def reduced(blocks):
            return feat_parts(jnp.sum(exchange(blocks).astype(single), axis=0))

        nothing = jnp.zeros((strengths, LANES), single)
        hessian_diag, *outs = call(
            lambda *refs: miss_body(scale, *refs),
            "miss",
            [((strengths, samples), single)] + [((far, strengths, width), single)] * near,
            *apply_rows(weights.astype(half), nothing), labels, design,
        )
        folded = outs[0]
        plane = {j: swap(outs[j].astype(jnp.float16), j) for j in reversed(range(1, near))}
        for j in range(1, near):
            folded = folded + plane[j].astype(single)
        received = swap_far(lambda k: folded[k].astype(jnp.float16))
        summed = folded[0]
        for k in range(1, far):
            summed = summed + received[k].astype(single)
        residual, square, blocks = call(
            gradient_body, "gradient", [field, scalars, ((samp, strengths, rank), half)],
            summed * (1.0 / scale), weights, lam, sketch,
        )
        direction, res_dot, block = call(
            first_body, "first", [field, scalars, spread], *reduced(blocks), lam, values, sketch, residual
        )
        update = weights
        for iteration in range(ITERS):
            parts = apply_rows(block, square)
            if iteration + 1 == ITERS:
                tiny = ((samp, SUBLANES, LANES), single)
                square, blocks = call(energy_body, "energy", [scalars, tiny], *parts, hessian_diag)
                return call(
                    finish_body, "finish", [field],
                    exchange(blocks), square, res_dot, lam, direction, update,
                )[0]
            shape = (far, strengths, width + LANES)
            square, *outs = call(
                image_body, "image", [scalars, (shape, single)] + [(shape, half)] * (near - 1),
                *parts, hessian_diag, design,
            )
            plane = {j: swap(outs[j], j) for j in reversed(range(1, near))}
            kept, *sent = call(
                lambda *refs: fold_body(near, *refs), "fold",
                [(shape[1:], single)] + [(shape[1:], half)] * (far - 1),
                outs[0], *[plane[j] for j in range(1, near)],
            )
            received = swap_far(lambda k: sent[k - 1])
            residual, update, res_dot, blocks = call(
                lambda *refs: step_body(far, *refs), "step",
                [field, field, scalars, ((samp, strengths, rank + LANES), half)],
                kept, *[received[k] for k in range(1, far)],
                square, res_dot, lam, direction, residual, update, sketch,
            )
            direction, res_dot, block = call(
                next_body, "next", [field, scalars, spread],
                *reduced(blocks), lam, values, sketch, residual, direction, res_dot,
            )
            square = nothing

    return shards


def solution(mesh):
    return jax.shard_map(
        make_shards(mesh.shape["samp"], mesh.shape["feat"]),
        mesh=mesh,
        in_specs=(
            P("samp", "feat"),
            P("samp"),
            P(None, ("feat", "samp")),
            P(),
            P(("feat", "samp"), None),
            P(),
        ),
        out_specs=P(None, ("feat", "samp")),
        check_vma=False,
    )
```

```python
import math

import jax
import jax.numpy as jnp
from jax import lax
from jax.experimental import pallas as pl
from jax.experimental.pallas import tpu as pltpu
from jax.sharding import PartitionSpec as P

LANES = 128
SUBLANES = 8
LARGEST = 0.09375
HALF_RANGE = 60000.0


def split(values):
    high = values.astype(jnp.bfloat16)
    rest = values - high.astype(jnp.float32)
    middle = rest.astype(jnp.bfloat16)
    low = (rest - middle.astype(jnp.float32)).astype(jnp.bfloat16)
    return high, middle, low


def exact_dot(values, other, contract):
    rows = values.shape[0]
    product = lax.dot_general(
        jnp.concatenate(split(values), axis=0),
        other,
        (((1,), (contract,)), ((), ())),
        preferred_element_type=jnp.float32,
    )
    return product[:rows] + product[rows : 2 * rows] + product[2 * rows :]


def pack(*columns_in):
    rows = columns_in[0].shape[0]
    lane = lax.broadcasted_iota(jnp.int32, (rows, LANES), 1)
    tile = jnp.zeros((rows, LANES), jnp.float32)
    for place, column in enumerate(columns_in):
        for index, part in enumerate(split(column)):
            tile = jnp.where(lane == 3 * place + index, part.astype(jnp.float32), tile)
    return tile


def unpack(tile, place):
    return jnp.sum(tile[:, 3 * place : 3 * place + 3], axis=1, keepdims=True)


def wide(column):
    return jnp.broadcast_to(column, (column.shape[0], LANES))


def repeat(out_ref, block):
    for part in range(out_ref.shape[0]):
        out_ref[part] = block


def load_body(offsets_ref, design_ref, out_ref, sems):
    parts = offsets_ref.shape[0]
    width = design_ref.shape[1] // parts
    copies = []
    for part in range(parts):
        offset = pl.multiple_of(offsets_ref[part], width)
        copies.append(
            pltpu.make_async_copy(
                design_ref.at[:, pl.ds(offset, width)],
                out_ref.at[:, pl.ds(part * width, width)],
                sems.at[part],
            )
        )
    for copy in copies:
        copy.start()
    for copy in copies:
        copy.wait()


def rows_body(near, *refs):
    *field_refs, design_ref, extra_ref, out_ref = refs
    whole_refs, old_refs = field_refs[:near], field_refs[near:]
    rows, strengths, width = whole_refs[0].shape
    samples = design_ref.shape[0]
    total = jnp.zeros((strengths, samples), jnp.float32)
    squares = jnp.zeros((strengths, width), jnp.float32)
    products = jnp.zeros((strengths, width), jnp.float32)
    part = 0
    for index, whole_ref in enumerate(whole_refs):
        for row in range(rows):
            block = whole_ref[row]
            total += lax.dot_general(
                block,
                design_ref[:, part * width : (part + 1) * width],
                (((1,), (1,)), ((), ())),
                preferred_element_type=jnp.float32,
            )
            values = block.astype(jnp.float32)
            squares += values * values
            if old_refs:
                products += values * old_refs[index][row].astype(jnp.float32)
            part += 1
    out_ref[:, :samples] = total
    lane = lax.broadcasted_iota(jnp.int32, (strengths, LANES), 1)
    tile = extra_ref[...]
    if old_refs:
        tile = jnp.where(lane == 1, jnp.sum(products, axis=1, keepdims=True), tile)
    out_ref[:, samples:] = jnp.where(lane == 0, jnp.sum(squares, axis=1, keepdims=True), tile)


def columns(values, design_ref, out_refs, scale=None):
    rows = out_refs[0].shape[0]
    width = design_ref.shape[1] // (rows * len(out_refs))
    part = 0
    for out_ref in out_refs:
        for row in range(rows):
            block = lax.dot_general(
                values,
                design_ref[:, part * width : (part + 1) * width],
                (((1,), (0,)), ((), ())),
                preferred_element_type=jnp.float32,
            )
            if scale is not None:
                block = block * scale
            out_ref[row, :, :width] = block.astype(out_ref.dtype)
            part += 1


def miss_body(scale, both_ref, other_ref, labels_ref, design_ref, hessian_ref, *out_refs):
    samples = design_ref.shape[0]
    logits = both_ref[:, :samples] + other_ref[:, :samples]
    probability = 1.0 / (1.0 + jnp.exp(-logits))
    hessian_ref[...] = probability * (1.0 - probability)
    miss_rows = (probability - labels_ref[...].astype(jnp.float32)).astype(jnp.bfloat16)
    columns(miss_rows, design_ref, out_refs, scale)


def tile_of(*columns_in):
    rows = columns_in[0].shape[0]
    lane = lax.broadcasted_iota(jnp.int32, (rows, LANES), 1)
    tile = jnp.zeros((rows, LANES), jnp.float32)
    for place, column in enumerate(columns_in):
        tile = jnp.where(lane == place, column, tile)
    return tile


def dot_of(first, second):
    return jnp.sum(first * second, axis=1, keepdims=True)


def ratios_of(lam_ref, values_ref):
    lam = lam_ref[:, :1]
    values = values_ref[...]
    smallest = jnp.min(values, axis=1, keepdims=True)
    return (smallest + lam) / (values + lam) - 1.0


def gradient_body(summed_ref, weights_ref, lam_ref, sketch_ref, residual_ref, payload_ref):
    residual = -(summed_ref[...] + lam_ref[:, :1] * weights_ref[...])
    residual_ref[...] = residual
    repeat(payload_ref, exact_dot(residual, sketch_ref[...], 0).astype(jnp.bfloat16))


def first_body(
    summed_ref, other_ref, lam_ref, values_ref, sketch_ref, residual_ref,
    direction_ref, projected_ref, half_ref,
):
    projected = summed_ref[...] + other_ref[...]
    projected_ref[...] = projected
    scaled = ratios_of(lam_ref, values_ref) * projected
    direction = residual_ref[...] + exact_dot(scaled, sketch_ref[...], 1)
    direction_ref[...] = direction
    half_ref[...] = direction.astype(jnp.bfloat16)


def image_of(image_rows, hessian_ref):
    return (hessian_ref[...] * image_rows).astype(jnp.bfloat16)


def image_body(both_ref, other_ref, hessian_ref, design_ref, rows_ref, scalars_ref, *out_refs):
    samples = hessian_ref.shape[1]
    both = both_ref[...] + other_ref[...]
    image_rows = both[:, :samples]
    rows_ref[...] = image_rows
    image = image_of(image_rows, hessian_ref)
    scalars_ref[...] = tile_of(
        both[:, samples : samples + 1], dot_of(image.astype(jnp.float32), image_rows)
    )
    columns(image, design_ref, out_refs)


def fold_body(near, *refs):
    own_ref, *received_refs = refs[:near]
    kept_ref, *sent_refs = refs[near:]
    for row, target_ref in enumerate([kept_ref] + sent_refs):
        total = own_ref[row]
        for received_ref in received_refs:
            total += received_ref[row].astype(jnp.float32)
        target_ref[...] = total.astype(target_ref.dtype)


def image_project_body(far, *refs):
    kept_ref, *received_refs = refs[:far]
    scalars_ref, lam_ref, direction_ref, residual_ref, sketch_ref, applied_ref, payload_ref = refs[far:]
    rank = sketch_ref.shape[1]
    summed = kept_ref[...]
    for received_ref in received_refs:
        summed += received_ref[...].astype(jnp.float32)
    applied = summed + lam_ref[:, :1] * direction_ref[...]
    applied_ref[...] = applied
    projected = exact_dot(applied, sketch_ref[...], 0).astype(jnp.bfloat16)
    residual = residual_ref[...]
    packed = pack(scalars_ref[:, 1:2], dot_of(residual, residual)).astype(jnp.bfloat16)
    for part in range(payload_ref.shape[0]):
        payload_ref[part, :, :rank] = projected
        payload_ref[part, :, rank:] = packed


def second_body(
    summed_ref, other_ref, lam_ref, values_ref, sketch_ref, scalars_ref, projected_ref,
    weights_ref, direction_ref, residual_ref, applied_ref,
    precond_ref, update_ref, known_ref, extra_ref, half_ref,
):
    rank = sketch_ref.shape[1]
    lam = lam_ref[:, :1]
    ratios = ratios_of(lam_ref, values_ref)
    projected = projected_ref[...]
    square = unpack(summed_ref[:, rank:] + other_ref[:, rank:], 1)
    energy = unpack(summed_ref[:, rank:], 0)
    res_dot = square + dot_of(ratios * projected, projected)
    step_size = res_dot / (energy + lam * scalars_ref[:, :1])
    residual = residual_ref[...] - step_size * applied_ref[...]
    projected = projected - step_size * (summed_ref[:, :rank] + other_ref[:, :rank])
    scaled = ratios * projected
    precond_res = residual + exact_dot(scaled, sketch_ref[...], 1)
    precond_ref[...] = precond_res
    half_ref[...] = precond_res.astype(jnp.bfloat16)
    update_ref[...] = weights_ref[...] + step_size * direction_ref[...]
    known_ref[...] = tile_of(res_dot, dot_of(scaled, projected), energy, scalars_ref[:, :1])
    zero = jnp.zeros_like(square)
    extra_ref[...] = tile_of(zero, zero, dot_of(residual, residual))


def energy_body(both_ref, other_ref, hessian_ref, rows_ref, squares_ref, payload_ref):
    samples = hessian_ref.shape[1]
    both = both_ref[...] + other_ref[...]
    squares_ref[...] = both[:, samples:]
    image_rows = both[:, :samples]
    image = image_of(image_rows, hessian_ref).astype(jnp.float32)
    sums = [dot_of(image, image_rows), dot_of(image, rows_ref[...]), both[:, samples + 2 : samples + 3]]
    lane = lax.broadcasted_iota(jnp.int32, (SUBLANES, LANES), 1)
    tile = jnp.zeros((SUBLANES, LANES), jnp.float32)
    for group in range(both.shape[0] // SUBLANES):
        for place, column in enumerate(sums):
            piece = column[group * SUBLANES : (group + 1) * SUBLANES]
            tile = jnp.where(lane == len(sums) * group + place, piece, tile)
    repeat(payload_ref, tile)


def finish_body(
    received_ref, squares_ref, known_ref, lam_ref, precond_ref, direction_ref, update_ref, out_ref
):
    tile = received_ref[0]
    for part in range(1, received_ref.shape[0]):
        tile += received_ref[part]
    groups = direction_ref.shape[0] // SUBLANES

    def total(place):
        lanes = [3 * group + place for group in range(groups)]
        return jnp.concatenate([tile[:, lane : lane + 1] for lane in lanes], axis=0)

    old_dot, part, old_energy, old_square = (known_ref[:, lane : lane + 1] for lane in range(4))
    res_dot = total(2) + part
    beta = res_dot / old_dot
    energy = total(0) + beta * (2.0 * total(1) + beta * old_energy)
    square = squares_ref[:, :1] + beta * (2.0 * squares_ref[:, 1:2] + beta * old_square)
    step_size = res_dot / (energy + lam_ref[:, :1] * square)
    direction = precond_ref[...] + beta * direction_ref[...]
    out_ref[...] = update_ref[...] + step_size * direction


VMEM = pl.BlockSpec(memory_space=pltpu.VMEM)


def call(body, name, shapes, *operands):
    return pl.pallas_call(
        body,
        out_shape=[jax.ShapeDtypeStruct(shape, dtype) for shape, dtype in shapes],
        in_specs=[VMEM] * len(operands),
        out_specs=[VMEM] * len(shapes),
        compiler_params=pltpu.CompilerParams(vmem_limit_bytes=8 << 20),
        name=name,
    )(*operands)


def load(design, offsets):
    return pl.pallas_call(
        load_body,
        out_shape=pltpu.VMEM(design.shape, design.dtype),
        in_specs=[pl.BlockSpec(memory_space=pltpu.SMEM), pl.BlockSpec(memory_space=pltpu.HBM)],
        out_specs=VMEM,
        scratch_shapes=[pltpu.SemaphoreType.DMA((offsets.shape[0],))],
        compiler_params=pltpu.CompilerParams(vmem_limit_bytes=1 << 20),
        name="load",
    )(offsets, design)


def make_shards(samp, feat):
    near = min(samp, 4)
    far = samp // near
    near_order = list(range(1, near))
    far_order = sorted(range(1, far), key=lambda distance: (distance * 2) % (far + 1))

    def swap(values, distance):
        return lax.ppermute(values, "samp", [(i, i ^ distance) for i in range(samp)])

    def gather(block):
        column = jnp.stack([block] + [swap(block, near * distance) for distance in far_order])
        return [column] + [swap(column, distance) for distance in near_order]

    def exchange(blocks):
        return lax.all_to_all(blocks, "samp", 0, 0)

    def feat_parts(values):
        if feat == 2:
            return values, lax.ppermute(values, "feat", [(0, 1), (1, 0)])
        return lax.psum(values, "feat"), jnp.zeros_like(values)

    def shards(design_matrix, labels, weights, lambdas, sketch, sketch_values):
        strengths, width = weights.shape
        samples = design_matrix.shape[0]
        rank = sketch.shape[1]
        single, half = jnp.float32, jnp.bfloat16
        field = ((strengths, width), single)
        scalars = ((strengths, LANES), single)
        spread = ((strengths, width), half)
        payload = ((samp, strengths, rank), half)
        wide_payload = ((samp, strengths, rank + LANES), half)
        scale = 2.0 ** math.floor(math.log2(HALF_RANGE / (samples * near * LARGEST)))
        lam = jnp.broadcast_to(lambdas[:, None], (strengths, LANES))
        labels = labels[None, :]
        values = sketch_values[None, :]
        places = [k * near + j for j in [0] + near_order for k in [0] + far_order]
        places = jnp.bitwise_xor(lax.axis_index("samp"), jnp.array(places, jnp.int32))
        if width % LANES == 0:
            design = load(design_matrix, places * width)
        else:
            design = design_matrix.reshape(samples, samp, width)
            design = jnp.take(design, places, axis=1).reshape(design_matrix.shape)

        def apply_rows(fields, extra):
            shape = ((strengths, samples + LANES), single)
            return feat_parts(
                call(lambda *refs: rows_body(near, *refs), "rows", [shape], *fields, design, extra)[0]
            )

        def reduced(blocks):
            return feat_parts(jnp.sum(exchange(blocks).astype(single), axis=0))

        nothing = jnp.zeros((strengths, LANES), single)
        start = lax.optimization_barrier(weights.astype(half))
        hessian_diag, *outs = call(
            lambda *refs: miss_body(scale, *refs),
            "miss",
            [((strengths, samples), single)] + [((far, strengths, width), single)] * near,
            *apply_rows(gather(start), nothing), labels, design,
        )
        folded = outs[0]
        for index, distance in enumerate(near_order):
            folded = folded + swap(outs[index + 1].astype(jnp.float16), distance).astype(single)
        summed = folded[0]
        for index, distance in enumerate(far_order):
            part = folded[index + 1].astype(jnp.float16)
            summed = summed + swap(part, near * distance).astype(single)
        residual, blocks = call(
            gradient_body, "gradient", [field, payload], summed * (1.0 / scale), weights, lam, sketch
        )
        direction, projected, block = call(
            first_body, "first", [field, ((strengths, rank), single), spread],
            *reduced(blocks), lam, values, sketch, residual,
        )
        whole = gather(block)
        shape = (far, strengths, width)
        image_rows, known, *outs = call(
            image_body, "image",
            [((strengths, samples), single), scalars, (shape, single)] + [(shape, half)] * (near - 1),
            *apply_rows(whole, nothing), hessian_diag, design,
        )
        kept, *sent = call(
            lambda *refs: fold_body(near, *refs), "fold", [field] + [spread] * (far - 1),
            outs[0], *[swap(out, distance) for out, distance in zip(outs[1:], near_order)],
        )
        applied, blocks = call(
            lambda *refs: image_project_body(far, *refs), "project", [field, wide_payload],
            kept, *[swap(part, near * distance) for part, distance in zip(sent, far_order)],
            known, lam, direction, residual, sketch,
        )
        precond_res, update, known, extra, block = call(
            second_body, "second", [field, field, scalars, scalars, spread],
            *reduced(blocks), lam, values, sketch, known, projected,
            weights, direction, residual, applied,
        )
        squares, blocks = call(
            energy_body, "energy", [scalars, ((samp, SUBLANES, LANES), single)],
            *apply_rows(gather(block) + whole, extra), hessian_diag, image_rows,
        )
        return call(
            finish_body, "finish", [field],
            exchange(blocks), squares, known, lam, precond_res, direction, update,
        )[0]

    return shards


def solution(mesh):
    return jax.shard_map(
        make_shards(mesh.shape["samp"], mesh.shape["feat"]),
        mesh=mesh,
        in_specs=(
            P("samp", "feat"),
            P("samp"),
            P(None, ("feat", "samp")),
            P(),
            P(("feat", "samp"), None),
            P(),
        ),
        out_specs=P(None, ("feat", "samp")),
        check_vma=False,
    )
```

```python
import math

import jax
import jax.numpy as jnp
from jax import lax
from jax.experimental import pallas as pl
from jax.experimental.pallas import tpu as pltpu
from jax.sharding import PartitionSpec as P


LANES = 128
SUBLANES = 8
LARGEST = 0.09375
HALF_RANGE = 60000.0


def split(values):
    high = values.astype(jnp.bfloat16)
    rest = values - high.astype(jnp.float32)
    middle = rest.astype(jnp.bfloat16)
    low = (rest - middle.astype(jnp.float32)).astype(jnp.bfloat16)
    return high, middle, low


def exact_dot(values, other, contract):
    rows = values.shape[0]
    product = lax.dot_general(
        jnp.concatenate(split(values), axis=0),
        other,
        (((1,), (contract,)), ((), ())),
        preferred_element_type=jnp.float32,
    )
    return product[:rows] + product[rows : 2 * rows] + product[2 * rows :]


def pack(*columns_in):
    rows = columns_in[0].shape[0]
    lane = lax.broadcasted_iota(jnp.int32, (rows, LANES), 1)
    tile = jnp.zeros((rows, LANES), jnp.float32)
    for place, column in enumerate(columns_in):
        for index, part in enumerate(split(column)):
            tile = jnp.where(lane == 3 * place + index, part.astype(jnp.float32), tile)
    return tile


def unpack(tile, place):
    return jnp.sum(tile[:, 3 * place : 3 * place + 3], axis=1, keepdims=True)


def repeat(out_ref, block):
    for part in range(out_ref.shape[0]):
        out_ref[part] = block


def load_body(offsets_ref, design_ref, out_ref, sems):
    parts = offsets_ref.shape[0]
    width = design_ref.shape[1] // parts
    copies = []
    for part in range(parts):
        offset = pl.multiple_of(offsets_ref[part], width)
        copies.append(
            pltpu.make_async_copy(
                design_ref.at[:, pl.ds(offset, width)],
                out_ref.at[:, pl.ds(part * width, width)],
                sems.at[part],
            )
        )
    for copy in copies:
        copy.start()
    for copy in copies:
        copy.wait()


def design_part(design_ref, place, width):
    return design_ref[:, place * width : (place + 1) * width]


def rows_body(places, again, *refs):
    *field_refs, design_ref, base_ref, out_ref = refs
    samples = design_ref.shape[0]
    blocks = []
    for field_ref in field_refs:
        if len(field_ref.shape) == 2:
            blocks.append(field_ref[...])
        else:
            blocks.extend(field_ref[row] for row in range(field_ref.shape[0]))
    strengths, width = blocks[0].shape
    total = jnp.zeros((strengths, samples), jnp.float32)
    squares = jnp.zeros((strengths, width), jnp.float32)
    products = jnp.zeros((strengths, width), jnp.float32)
    for index, place in enumerate(places):
        total += lax.dot_general(
            blocks[index],
            design_part(design_ref, place, width),
            (((1,), (1,)), ((), ())),
            preferred_element_type=jnp.float32,
        )
        values = blocks[index].astype(jnp.float32)
        squares += values * values
        if again:
            products += values * blocks[len(places) + index].astype(jnp.float32)
    square = jnp.sum(squares, axis=1, keepdims=True)
    sums = [square, jnp.sum(products, axis=1, keepdims=True)] if again else [square]
    base = base_ref[...]
    if base.shape[1] > LANES:
        out_ref[:, :samples] = base[:, :samples] + total
        out_ref[:, samples:] = base[:, samples:] + tile_of(*sums)
    else:
        out_ref[:, :samples] = total
        out_ref[:, samples:] = base + tile_of(*sums)


def columns(values, design_ref, places, out_refs, scale=None):
    targets = []
    for out_ref in out_refs:
        if len(out_ref.shape) == 2:
            targets.append((out_ref, ...))
        else:
            targets.extend((out_ref, row) for row in range(out_ref.shape[0]))
    for place, (out_ref, row) in zip(places, targets):
        block = lax.dot_general(
            values,
            design_part(design_ref, place, out_ref.shape[-1]),
            (((1,), (0,)), ((), ())),
            preferred_element_type=jnp.float32,
        )
        if scale is not None:
            block = block * scale
        out_ref[row] = block.astype(out_ref.dtype)


def miss_body(scale, places, both_ref, other_ref, labels_ref, design_ref, hessian_ref, miss_ref, *out_refs):
    samples = design_ref.shape[0]
    logits = both_ref[:, :samples] + other_ref[:, :samples]
    probability = 1.0 / (1.0 + jnp.exp(-logits))
    hessian_ref[...] = probability * (1.0 - probability)
    miss_rows = (probability - labels_ref[...].astype(jnp.float32)).astype(jnp.bfloat16)
    miss_ref[...] = miss_rows
    columns(miss_rows, design_ref, places, out_refs, scale)


def more_body(scale, places, values_ref, design_ref, *out_refs):
    columns(values_ref[...], design_ref, places, out_refs, scale)


def tile_of(*columns_in):
    rows = columns_in[0].shape[0]
    lane = lax.broadcasted_iota(jnp.int32, (rows, LANES), 1)
    tile = jnp.zeros((rows, LANES), jnp.float32)
    for place, column in enumerate(columns_in):
        tile = jnp.where(lane == place, column, tile)
    return tile


def dot_of(first, second):
    return jnp.sum(first * second, axis=1, keepdims=True)


def ratios_of(lam_ref, values_ref):
    lam = lam_ref[:, :1]
    values = values_ref[...]
    smallest = jnp.min(values, axis=1, keepdims=True)
    return (smallest + lam) / (values + lam) - 1.0


def gradient_body(summed_ref, weights_ref, lam_ref, sketch_ref, residual_ref, payload_ref):
    residual = -(summed_ref[...] + lam_ref[:, :1] * weights_ref[...])
    residual_ref[...] = residual
    repeat(payload_ref, exact_dot(residual, sketch_ref[...], 0).astype(jnp.bfloat16))


def first_body(
    summed_ref, other_ref, lam_ref, values_ref, sketch_ref, residual_ref,
    direction_ref, projected_ref, half_ref,
):
    projected = summed_ref[...] + other_ref[...]
    projected_ref[...] = projected
    scaled = ratios_of(lam_ref, values_ref) * projected
    direction = residual_ref[...] + exact_dot(scaled, sketch_ref[...], 1)
    direction_ref[...] = direction
    half_ref[...] = direction.astype(jnp.bfloat16)


def image_of(image_rows, hessian_ref):
    return (hessian_ref[...] * image_rows).astype(jnp.bfloat16)


def image_body(
    places, both_ref, other_ref, hessian_ref, design_ref, rows_ref, image_ref, scalars_ref, *out_refs
):
    samples = hessian_ref.shape[1]
    both = both_ref[...] + other_ref[...]
    image_rows = both[:, :samples]
    rows_ref[...] = image_rows
    image = image_of(image_rows, hessian_ref)
    image_ref[...] = image
    scalars_ref[...] = tile_of(
        both[:, samples : samples + 1], dot_of(image.astype(jnp.float32), image_rows)
    )
    columns(image, design_ref, places, out_refs)


def fold_body(own_ref, *refs):
    count = own_ref.shape[0]
    received_refs, target_refs = refs[:-count], refs[-count:]
    for row, target_ref in enumerate(target_refs):
        total = own_ref[row]
        for received_ref in received_refs:
            total += received_ref[row].astype(jnp.float32)
        target_ref[...] = total.astype(target_ref.dtype)


def image_project_body(count, own_ref, *refs):
    received_refs = refs[:count]
    scalars_ref, lam_ref, direction_ref, residual_ref, sketch_ref, applied_ref, payload_ref = refs[count:]
    rank = sketch_ref.shape[1]
    summed = own_ref[...]
    for received_ref in received_refs:
        summed += received_ref[...].astype(jnp.float32)
    applied = summed + lam_ref[:, :1] * direction_ref[...]
    applied_ref[...] = applied
    projected = exact_dot(applied, sketch_ref[...], 0).astype(jnp.bfloat16)
    residual = residual_ref[...]
    packed = pack(scalars_ref[:, 1:2], dot_of(residual, residual)).astype(jnp.bfloat16)
    for part in range(payload_ref.shape[0]):
        payload_ref[part, :, :rank] = projected
        payload_ref[part, :, rank:] = packed


def second_body(
    summed_ref, other_ref, lam_ref, values_ref, sketch_ref, scalars_ref, projected_ref,
    weights_ref, direction_ref, residual_ref, applied_ref,
    precond_ref, update_ref, known_ref, extra_ref, half_ref,
):
    rank = sketch_ref.shape[1]
    lam = lam_ref[:, :1]
    ratios = ratios_of(lam_ref, values_ref)
    projected = projected_ref[...]
    square = unpack(summed_ref[:, rank:] + other_ref[:, rank:], 1)
    energy = unpack(summed_ref[:, rank:], 0)
    res_dot = square + dot_of(ratios * projected, projected)
    step_size = res_dot / (energy + lam * scalars_ref[:, :1])
    residual = residual_ref[...] - step_size * applied_ref[...]
    projected = projected - step_size * (summed_ref[:, :rank] + other_ref[:, :rank])
    scaled = ratios * projected
    precond_res = residual + exact_dot(scaled, sketch_ref[...], 1)
    precond_ref[...] = precond_res
    half_ref[...] = precond_res.astype(jnp.bfloat16)
    update_ref[...] = weights_ref[...] + step_size * direction_ref[...]
    known_ref[...] = tile_of(res_dot, dot_of(scaled, projected), energy, scalars_ref[:, :1])
    zero = jnp.zeros_like(square)
    extra_ref[...] = tile_of(zero, zero, dot_of(residual, residual))


def energy_body(both_ref, other_ref, hessian_ref, rows_ref, squares_ref, payload_ref):
    samples = hessian_ref.shape[1]
    both = both_ref[...] + other_ref[...]
    squares_ref[...] = both[:, samples:]
    image_rows = both[:, :samples]
    image = image_of(image_rows, hessian_ref).astype(jnp.float32)
    sums = [dot_of(image, image_rows), dot_of(image, rows_ref[...]), both[:, samples + 2 : samples + 3]]
    lane = lax.broadcasted_iota(jnp.int32, (SUBLANES, LANES), 1)
    tile = jnp.zeros((SUBLANES, LANES), jnp.float32)
    for group in range(both.shape[0] // SUBLANES):
        for place, column in enumerate(sums):
            piece = column[group * SUBLANES : (group + 1) * SUBLANES]
            tile = jnp.where(lane == len(sums) * group + place, piece, tile)
    repeat(payload_ref, tile)


def finish_body(
    received_ref, squares_ref, known_ref, lam_ref, precond_ref, direction_ref, update_ref, out_ref
):
    tile = received_ref[0]
    for part in range(1, received_ref.shape[0]):
        tile += received_ref[part]
    groups = direction_ref.shape[0] // SUBLANES

    def total(place):
        lanes = [3 * group + place for group in range(groups)]
        return jnp.concatenate([tile[:, lane : lane + 1] for lane in lanes], axis=0)

    old_dot, part, old_energy, old_square = (known_ref[:, lane : lane + 1] for lane in range(4))
    res_dot = total(2) + part
    beta = res_dot / old_dot
    energy = total(0) + beta * (2.0 * total(1) + beta * old_energy)
    square = squares_ref[:, :1] + beta * (2.0 * squares_ref[:, 1:2] + beta * old_square)
    step_size = res_dot / (energy + lam_ref[:, :1] * square)
    direction = precond_ref[...] + beta * direction_ref[...]
    out_ref[...] = update_ref[...] + step_size * direction


VMEM = pl.BlockSpec(memory_space=pltpu.VMEM)


def call(body, shapes, *operands):
    return pl.pallas_call(
        body,
        out_shape=[jax.ShapeDtypeStruct(shape, dtype) for shape, dtype in shapes],
        in_specs=[VMEM] * len(operands),
        out_specs=[VMEM] * len(shapes),
        compiler_params=pltpu.CompilerParams(vmem_limit_bytes=8 << 20),
    )(*operands)


def load(design, offsets):
    return pl.pallas_call(
        load_body,
        out_shape=pltpu.VMEM(design.shape, design.dtype),
        in_specs=[pl.BlockSpec(memory_space=pltpu.SMEM), pl.BlockSpec(memory_space=pltpu.HBM)],
        out_specs=VMEM,
        scratch_shapes=[pltpu.SemaphoreType.DMA((offsets.shape[0],))],
        compiler_params=pltpu.CompilerParams(vmem_limit_bytes=1 << 20),
        name="load",
    )(offsets, design)


def make_shards(samp, feat):
    near = min(samp, 4)
    far = samp // near
    near_order = list(range(1, near))
    far_order = sorted(range(1, far), key=lambda distance: (distance * 2) % (far + 1))

    def swap(values, distance):
        return lax.ppermute(values, "samp", [(i, i ^ distance) for i in range(samp)])

    def swap_far(values):
        received = []
        for value, distance in zip(values, far_order):
            received.append(swap(value, near * distance))
        return received

    def swap_near(values):
        return [swap(value, distance) for value, distance in zip(values, near_order)]

    def gather(block):
        column = jnp.stack([block] + swap_far([block] * len(far_order)))
        return [column], swap_near([column] * len(near_order))

    def exchange(blocks):
        return lax.all_to_all(blocks, "samp", 0, 0)

    def feat_parts(values):
        if feat == 2:
            return values, lax.ppermute(values, "feat", [(0, 1), (1, 0)])
        return lax.psum(values, "feat"), jnp.zeros_like(values)

    def shards(design_matrix, labels, weights, lambdas, sketch, sketch_values):
        strengths, width = weights.shape
        samples = design_matrix.shape[0]
        rank = sketch.shape[1]
        single, half = jnp.float32, jnp.bfloat16
        field = ((strengths, width), single)
        scalars = ((strengths, LANES), single)
        spread = ((strengths, width), half)
        payload = ((samp, strengths, rank), half)
        wide_payload = ((samp, strengths, rank + LANES), half)
        scale = 2.0 ** math.floor(math.log2(HALF_RANGE / (samples * near * LARGEST)))
        lam = jnp.broadcast_to(lambdas[:, None], (strengths, LANES))
        labels = labels[None, :]
        values = sketch_values[None, :]
        places = [k * near + j for j in [0] + near_order for k in [0] + far_order]
        places = jnp.bitwise_xor(lax.axis_index("samp"), jnp.array(places, jnp.int32))
        if width % LANES == 0:
            design = load(design_matrix, places * width)
        else:
            design = design_matrix.reshape(samples, samp, width)
            design = jnp.take(design, places, axis=1).reshape(design_matrix.shape)

        column_places = list(range(far))
        plane_places = list(range(far, samp))

        def apply_rows(fields, earlier, base):
            both = base
            for places, blocks, old in zip((column_places, plane_places), fields, earlier):
                both = call(
                    lambda *refs: rows_body(places, len(old) > 0, *refs),
                    [((strengths, samples + LANES), single)], *blocks, *old, design, both,
                )[0]
            return feat_parts(both)

        def reduced(blocks):
            return feat_parts(jnp.sum(exchange(blocks).astype(single), axis=0))

        nothing = jnp.zeros((strengths, LANES), single)
        start = lax.optimization_barrier(weights.astype(half))
        sample_field = (strengths, samples)
        column = (far, strengths, width)
        hessian_diag, miss_rows, *outs = call(
            lambda *refs: miss_body(scale, plane_places, *refs),
            [(sample_field, single), (sample_field, half)] + [(column, single)] * (near - 1),
            *apply_rows(gather(start), ([], []), nothing), labels, design,
        )
        folded = call(
            lambda *refs: more_body(scale, column_places, *refs),
            [(column, single)], miss_rows, design,
        )[0]
        for received in swap_near([out.astype(jnp.float16) for out in outs]):
            folded = folded + received.astype(single)
        summed = folded[0]
        for received in swap_far([folded[k].astype(jnp.float16) for k in range(1, far)]):
            summed = summed + received.astype(single)
        residual, blocks = call(
            gradient_body, [field, payload], summed * (1.0 / scale), weights, lam, sketch
        )
        direction, projected, block = call(
            first_body, [field, ((strengths, rank), single), spread],
            *reduced(blocks), lam, values, sketch, residual,
        )
        whole = gather(block)
        image_rows, image, known, *outs = call(
            lambda *refs: image_body(plane_places, *refs),
            [(sample_field, single), (sample_field, half), scalars] + [(column, half)] * (near - 1),
            *apply_rows(whole, ([], []), nothing), hessian_diag, design,
        )
        own = call(
            lambda *refs: more_body(None, column_places, *refs),
            [(column, single)], image, design,
        )[0]
        kept, *sent = call(fold_body, [field] + [spread] * (far - 1), own, *swap_near(outs))
        applied, blocks = call(
            lambda *refs: image_project_body(far - 1, *refs), [field, wide_payload],
            kept, *swap_far(sent), known, lam, direction, residual, sketch,
        )
        precond_res, update, known, extra, block = call(
            second_body, [field, field, scalars, scalars, spread],
            *reduced(blocks), lam, values, sketch, known, projected,
            weights, direction, residual, applied,
        )
        squares, blocks = call(
            energy_body, [scalars, ((samp, SUBLANES, LANES), single)],
            *apply_rows(gather(block), whole, extra), hessian_diag, image_rows,
        )
        return call(
            finish_body, [field],
            exchange(blocks), squares, known, lam, precond_res, direction, update,
        )[0]

    return shards


def solution(mesh):
    return jax.shard_map(
        make_shards(mesh.shape["samp"], mesh.shape["feat"]),
        mesh=mesh,
        in_specs=(
            P("samp", "feat"),
            P("samp"),
            P(None, ("feat", "samp")),
            P(),
            P(("feat", "samp"), None),
            P(),
        ),
        out_specs=P(None, ("feat", "samp")),
        check_vma=False,
    )
```

```python
import math

import jax
import jax.numpy as jnp
from jax import lax
from jax.experimental import pallas as pl
from jax.experimental.pallas import tpu as pltpu
from jax.sharding import PartitionSpec as P


LANES = 128
SUBLANES = 8
LARGEST = 0.09375
HALF_RANGE = 60000.0


def split(values):
    high = values.astype(jnp.bfloat16)
    rest = values - high.astype(jnp.float32)
    middle = rest.astype(jnp.bfloat16)
    low = (rest - middle.astype(jnp.float32)).astype(jnp.bfloat16)
    return high, middle, low


def exact_dot(values, other, contract):
    rows = values.shape[0]
    product = lax.dot_general(
        jnp.concatenate(split(values), axis=0),
        other,
        (((1,), (contract,)), ((), ())),
        preferred_element_type=jnp.float32,
    )
    return product[:rows] + product[rows : 2 * rows] + product[2 * rows :]


def pack(*columns_in):
    rows = columns_in[0].shape[0]
    lane = lax.broadcasted_iota(jnp.int32, (rows, LANES), 1)
    tile = jnp.zeros((rows, LANES), jnp.float32)
    for place, column in enumerate(columns_in):
        for index, part in enumerate(split(column)):
            tile = jnp.where(lane == 3 * place + index, part.astype(jnp.float32), tile)
    return tile


def unpack(tile, place):
    return jnp.sum(tile[:, 3 * place : 3 * place + 3], axis=1, keepdims=True)


def repeat(out_ref, block):
    for part in range(out_ref.shape[0]):
        out_ref[part] = block


def load_body(offsets_ref, design_ref, out_ref, sems):
    parts = offsets_ref.shape[0]
    width = design_ref.shape[1] // parts
    copies = []
    for part in range(parts):
        offset = pl.multiple_of(offsets_ref[part], width)
        copies.append(
            pltpu.make_async_copy(
                design_ref.at[:, pl.ds(offset, width)],
                out_ref.at[:, pl.ds(part * width, width)],
                sems.at[part],
            )
        )
    for copy in copies:
        copy.start()
    for copy in copies:
        copy.wait()


def design_part(design_ref, place, width):
    return design_ref[:, place * width : (place + 1) * width]


def rows_body(places, again, *refs):
    *field_refs, design_ref, base_ref, out_ref = refs
    samples = design_ref.shape[0]
    blocks = []
    for field_ref in field_refs:
        if len(field_ref.shape) == 2:
            blocks.append(field_ref[...])
        else:
            blocks.extend(field_ref[row] for row in range(field_ref.shape[0]))
    strengths, width = blocks[0].shape
    total = jnp.zeros((strengths, samples), jnp.float32)
    squares = jnp.zeros((strengths, width), jnp.float32)
    products = jnp.zeros((strengths, width), jnp.float32)
    for index, place in enumerate(places):
        total += lax.dot_general(
            blocks[index],
            design_part(design_ref, place, width),
            (((1,), (1,)), ((), ())),
            preferred_element_type=jnp.float32,
        )
        values = blocks[index].astype(jnp.float32)
        squares += values * values
        if again:
            products += values * blocks[len(places) + index].astype(jnp.float32)
    square = jnp.sum(squares, axis=1, keepdims=True)
    sums = [square, jnp.sum(products, axis=1, keepdims=True)] if again else [square]
    base = base_ref[...]
    if base.shape[1] > LANES:
        out_ref[:, :samples] = base[:, :samples] + total
        out_ref[:, samples:] = base[:, samples:] + tile_of(*sums)
    else:
        out_ref[:, :samples] = total
        out_ref[:, samples:] = base + tile_of(*sums)


def columns(values, design_ref, places, out_refs, scale=None):
    targets = []
    for out_ref in out_refs:
        if len(out_ref.shape) == 2:
            targets.append((out_ref, ...))
        else:
            targets.extend((out_ref, row) for row in range(out_ref.shape[0]))
    for place, (out_ref, row) in zip(places, targets):
        block = lax.dot_general(
            values,
            design_part(design_ref, place, out_ref.shape[-1]),
            (((1,), (0,)), ((), ())),
            preferred_element_type=jnp.float32,
        )
        if scale is not None:
            block = block * scale
        out_ref[row] = block.astype(out_ref.dtype)


def miss_body(scale, places, both_ref, other_ref, labels_ref, design_ref, hessian_ref, miss_ref, *out_refs):
    samples = design_ref.shape[0]
    logits = both_ref[:, :samples] + other_ref[:, :samples]
    probability = 1.0 / (1.0 + jnp.exp(-logits))
    hessian_ref[...] = probability * (1.0 - probability)
    miss_rows = (probability - labels_ref[...].astype(jnp.float32)).astype(jnp.bfloat16)
    miss_ref[...] = miss_rows
    columns(miss_rows, design_ref, places, out_refs, scale)


def more_body(scale, places, values_ref, design_ref, *out_refs):
    columns(values_ref[...], design_ref, places, out_refs, scale)


def tile_of(*columns_in):
    rows = columns_in[0].shape[0]
    lane = lax.broadcasted_iota(jnp.int32, (rows, LANES), 1)
    tile = jnp.zeros((rows, LANES), jnp.float32)
    for place, column in enumerate(columns_in):
        tile = jnp.where(lane == place, column, tile)
    return tile


def dot_of(first, second):
    return jnp.sum(first * second, axis=1, keepdims=True)


def ratios_of(lam_ref, values_ref):
    lam = lam_ref[:, :1]
    values = values_ref[...]
    smallest = jnp.min(values, axis=1, keepdims=True)
    return (smallest + lam) / (values + lam) - 1.0


def gradient_body(summed_ref, weights_ref, lam_ref, sketch_ref, residual_ref, payload_ref):
    residual = -(summed_ref[...] + lam_ref[:, :1] * weights_ref[...])
    residual_ref[...] = residual
    repeat(payload_ref, exact_dot(residual, sketch_ref[...], 0).astype(jnp.bfloat16))


def first_body(
    summed_ref, other_ref, lam_ref, values_ref, sketch_ref, residual_ref,
    direction_ref, projected_ref, half_ref,
):
    projected = summed_ref[...] + other_ref[...]
    projected_ref[...] = projected
    scaled = ratios_of(lam_ref, values_ref) * projected
    direction = residual_ref[...] + exact_dot(scaled, sketch_ref[...], 1)
    direction_ref[...] = direction
    half_ref[...] = direction.astype(jnp.bfloat16)


def image_of(image_rows, hessian_ref):
    return (hessian_ref[...] * image_rows).astype(jnp.bfloat16)


def image_body(
    places, both_ref, other_ref, hessian_ref, design_ref, rows_ref, image_ref, scalars_ref, *out_refs
):
    samples = hessian_ref.shape[1]
    both = both_ref[...] + other_ref[...]
    image_rows = both[:, :samples]
    rows_ref[...] = image_rows
    image = image_of(image_rows, hessian_ref)
    image_ref[...] = image
    scalars_ref[...] = tile_of(
        both[:, samples : samples + 1], dot_of(image.astype(jnp.float32), image_rows)
    )
    columns(image, design_ref, places, out_refs)


def fold_body(own_ref, *refs):
    count = own_ref.shape[0]
    received_refs, target_refs = refs[:-count], refs[-count:]
    for row, target_ref in enumerate(target_refs):
        total = own_ref[row]
        for received_ref in received_refs:
            total += received_ref[row].astype(jnp.float32)
        target_ref[...] = total.astype(target_ref.dtype)


def image_project_body(count, own_ref, *refs):
    received_refs = refs[:count]
    scalars_ref, lam_ref, direction_ref, residual_ref, sketch_ref, applied_ref, payload_ref = refs[count:]
    rank = sketch_ref.shape[1]
    summed = own_ref[...]
    for received_ref in received_refs:
        summed += received_ref[...].astype(jnp.float32)
    applied = summed + lam_ref[:, :1] * direction_ref[...]
    applied_ref[...] = applied
    projected = exact_dot(applied, sketch_ref[...], 0).astype(jnp.bfloat16)
    residual = residual_ref[...]
    packed = pack(scalars_ref[:, 1:2], dot_of(residual, residual)).astype(jnp.bfloat16)
    for part in range(payload_ref.shape[0]):
        payload_ref[part, :, :rank] = projected
        payload_ref[part, :, rank:] = packed


def second_body(
    summed_ref, other_ref, lam_ref, values_ref, sketch_ref, scalars_ref, projected_ref,
    weights_ref, direction_ref, residual_ref, applied_ref,
    precond_ref, update_ref, known_ref, extra_ref, half_ref,
):
    rank = sketch_ref.shape[1]
    lam = lam_ref[:, :1]
    ratios = ratios_of(lam_ref, values_ref)
    projected = projected_ref[...]
    square = unpack(summed_ref[:, rank:] + other_ref[:, rank:], 1)
    energy = unpack(summed_ref[:, rank:], 0)
    res_dot = square + dot_of(ratios * projected, projected)
    step_size = res_dot / (energy + lam * scalars_ref[:, :1])
    residual = residual_ref[...] - step_size * applied_ref[...]
    projected = projected - step_size * (summed_ref[:, :rank] + other_ref[:, :rank])
    scaled = ratios * projected
    precond_res = residual + exact_dot(scaled, sketch_ref[...], 1)
    precond_ref[...] = precond_res
    half_ref[...] = precond_res.astype(jnp.bfloat16)
    update_ref[...] = weights_ref[...] + step_size * direction_ref[...]
    known_ref[...] = tile_of(res_dot, dot_of(scaled, projected), energy, scalars_ref[:, :1])
    zero = jnp.zeros_like(square)
    extra_ref[...] = tile_of(zero, zero, dot_of(residual, residual))


def energy_body(both_ref, other_ref, hessian_ref, rows_ref, squares_ref, payload_ref):
    samples = hessian_ref.shape[1]
    both = both_ref[...] + other_ref[...]
    squares_ref[...] = both[:, samples:]
    image_rows = both[:, :samples]
    image = image_of(image_rows, hessian_ref).astype(jnp.float32)
    sums = [dot_of(image, image_rows), dot_of(image, rows_ref[...]), both[:, samples + 2 : samples + 3]]
    lane = lax.broadcasted_iota(jnp.int32, (SUBLANES, LANES), 1)
    tile = jnp.zeros((SUBLANES, LANES), jnp.float32)
    for group in range(both.shape[0] // SUBLANES):
        for place, column in enumerate(sums):
            piece = column[group * SUBLANES : (group + 1) * SUBLANES]
            tile = jnp.where(lane == len(sums) * group + place, piece, tile)
    repeat(payload_ref, tile)


def finish_body(
    received_ref, squares_ref, known_ref, lam_ref, precond_ref, direction_ref, update_ref, out_ref
):
    tile = received_ref[0]
    for part in range(1, received_ref.shape[0]):
        tile += received_ref[part]
    groups = direction_ref.shape[0] // SUBLANES

    def total(place):
        lanes = [3 * group + place for group in range(groups)]
        return jnp.concatenate([tile[:, lane : lane + 1] for lane in lanes], axis=0)

    old_dot, part, old_energy, old_square = (known_ref[:, lane : lane + 1] for lane in range(4))
    res_dot = total(2) + part
    beta = res_dot / old_dot
    energy = total(0) + beta * (2.0 * total(1) + beta * old_energy)
    square = squares_ref[:, :1] + beta * (2.0 * squares_ref[:, 1:2] + beta * old_square)
    step_size = res_dot / (energy + lam_ref[:, :1] * square)
    direction = precond_ref[...] + beta * direction_ref[...]
    out_ref[...] = update_ref[...] + step_size * direction


VMEM = pl.BlockSpec(memory_space=pltpu.VMEM)


def call(body, shapes, *operands):
    return pl.pallas_call(
        body,
        out_shape=[jax.ShapeDtypeStruct(shape, dtype) for shape, dtype in shapes],
        in_specs=[VMEM] * len(operands),
        out_specs=[VMEM] * len(shapes),
        compiler_params=pltpu.CompilerParams(vmem_limit_bytes=8 << 20),
    )(*operands)


def load(design, offsets):
    return pl.pallas_call(
        load_body,
        out_shape=pltpu.VMEM(design.shape, design.dtype),
        in_specs=[pl.BlockSpec(memory_space=pltpu.SMEM), pl.BlockSpec(memory_space=pltpu.HBM)],
        out_specs=VMEM,
        scratch_shapes=[pltpu.SemaphoreType.DMA((offsets.shape[0],))],
        compiler_params=pltpu.CompilerParams(vmem_limit_bytes=1 << 20),
        name="load",
    )(offsets, design)


def make_shards(samp, feat):
    near = min(samp, 4)
    far = samp // near
    near_order = list(range(1, near))
    far_order = sorted(range(1, far), key=lambda distance: (distance * 2) % (far + 1))

    def swap(values, distance):
        return lax.ppermute(values, "samp", [(i, i ^ distance) for i in range(samp)])

    def swap_far(values):
        received = []
        for value, distance in zip(values, far_order):
            received.append(swap(value, near * distance))
        return received

    def swap_near(values):
        received = []
        for value, distance in zip(values, near_order):
            received.append(swap(value, distance))
        return received

    def gather(block):
        column = jnp.stack([block] + swap_far([block] * len(far_order)))
        return [column], swap_near([column] * len(near_order))

    def exchange(blocks):
        return lax.all_to_all(blocks, "samp", 0, 0)

    def feat_parts(values):
        if feat == 2:
            return values, lax.ppermute(values, "feat", [(0, 1), (1, 0)])
        return lax.psum(values, "feat"), jnp.zeros_like(values)

    def shards(design_matrix, labels, weights, lambdas, sketch, sketch_values):
        strengths, width = weights.shape
        samples = design_matrix.shape[0]
        rank = sketch.shape[1]
        single, half = jnp.float32, jnp.bfloat16
        field = ((strengths, width), single)
        scalars = ((strengths, LANES), single)
        spread = ((strengths, width), half)
        payload = ((samp, strengths, rank), half)
        wide_payload = ((samp, strengths, rank + LANES), half)
        scale = 2.0 ** math.floor(math.log2(HALF_RANGE / (samples * near * LARGEST)))
        lam = jnp.broadcast_to(lambdas[:, None], (strengths, LANES))
        labels = labels[None, :]
        values = sketch_values[None, :]
        places = [k * near + j for j in [0] + near_order for k in [0] + far_order]
        places = jnp.bitwise_xor(lax.axis_index("samp"), jnp.array(places, jnp.int32))
        if width % LANES == 0:
            design = load(design_matrix, places * width)
        else:
            design = design_matrix.reshape(samples, samp, width)
            design = jnp.take(design, places, axis=1).reshape(design_matrix.shape)

        column_places = list(range(far))
        plane_places = list(range(far, samp))

        def apply_rows(fields, earlier, base):
            both = base
            for places, blocks, old in zip((column_places, plane_places), fields, earlier):
                both = call(
                    lambda *refs: rows_body(places, len(old) > 0, *refs),
                    [((strengths, samples + LANES), single)], *blocks, *old, design, both,
                )[0]
            return feat_parts(both)

        def reduced(blocks):
            return feat_parts(jnp.sum(exchange(blocks).astype(single), axis=0))

        nothing = jnp.zeros((strengths, LANES), single)
        start = lax.optimization_barrier(weights.astype(half))
        sample_field = (strengths, samples)
        column = (far, strengths, width)
        hessian_diag, miss_rows, *outs = call(
            lambda *refs: miss_body(scale, plane_places, *refs),
            [(sample_field, single), (sample_field, half)] + [(column, single)] * (near - 1),
            *apply_rows(gather(start), ([], []), nothing), labels, design,
        )
        folded = call(
            lambda *refs: more_body(scale, column_places, *refs),
            [(column, single)], miss_rows, design,
        )[0]
        for received in swap_near([out.astype(jnp.float16) for out in outs]):
            folded = folded + received.astype(single)
        summed = folded[0]
        for received in swap_far([folded[k].astype(jnp.float16) for k in range(1, far)]):
            summed = summed + received.astype(single)
        residual, blocks = call(
            gradient_body, [field, payload], summed * (1.0 / scale), weights, lam, sketch
        )
        direction, projected, block = call(
            first_body, [field, ((strengths, rank), single), spread],
            *reduced(blocks), lam, values, sketch, residual,
        )
        whole = gather(block)
        image_rows, image, known, *outs = call(
            lambda *refs: image_body(plane_places, *refs),
            [(sample_field, single), (sample_field, half), scalars] + [(column, half)] * (near - 1),
            *apply_rows(whole, ([], []), nothing), hessian_diag, design,
        )
        own = call(
            lambda *refs: more_body(None, column_places, *refs),
            [(column, single)], image, design,
        )[0]
        kept, *sent = call(fold_body, [field] + [spread] * (far - 1), own, *swap_near(outs))
        applied, blocks = call(
            lambda *refs: image_project_body(far - 1, *refs), [field, wide_payload],
            kept, *swap_far(sent), known, lam, direction, residual, sketch,
        )
        precond_res, update, known, extra, block = call(
            second_body, [field, field, scalars, scalars, spread],
            *reduced(blocks), lam, values, sketch, known, projected,
            weights, direction, residual, applied,
        )
        squares, blocks = call(
            energy_body, [scalars, ((samp, SUBLANES, LANES), single)],
            *apply_rows(gather(block), whole, extra), hessian_diag, image_rows,
        )
        return call(
            finish_body, [field],
            exchange(blocks), squares, known, lam, precond_res, direction, update,
        )[0]

    return shards


def solution(mesh):
    return jax.shard_map(
        make_shards(mesh.shape["samp"], mesh.shape["feat"]),
        mesh=mesh,
        in_specs=(
            P("samp", "feat"),
            P("samp"),
            P(None, ("feat", "samp")),
            P(),
            P(("feat", "samp"), None),
            P(),
        ),
        out_specs=P(None, ("feat", "samp")),
        check_vma=False,
    )
```

```python
import math

import jax
import jax.numpy as jnp
from jax import lax
from jax.experimental import pallas as pl
from jax.experimental.pallas import tpu as pltpu
from jax.sharding import PartitionSpec as P


LANES = 128
SUBLANES = 8
LARGEST = 0.09375
HALF_RANGE = 60000.0


def split(values):
    high = values.astype(jnp.bfloat16)
    rest = values - high.astype(jnp.float32)
    middle = rest.astype(jnp.bfloat16)
    low = (rest - middle.astype(jnp.float32)).astype(jnp.bfloat16)
    return high, middle, low


def exact_dot(values, other, contract):
    rows = values.shape[0]
    product = lax.dot_general(
        jnp.concatenate(split(values), axis=0),
        other,
        (((1,), (contract,)), ((), ())),
        preferred_element_type=jnp.float32,
    )
    return product[:rows] + product[rows : 2 * rows] + product[2 * rows :]


def pack(*columns_in):
    rows = columns_in[0].shape[0]
    lane = lax.broadcasted_iota(jnp.int32, (rows, LANES), 1)
    tile = jnp.zeros((rows, LANES), jnp.float32)
    for place, column in enumerate(columns_in):
        for index, part in enumerate(split(column)):
            tile = jnp.where(lane == 3 * place + index, part.astype(jnp.float32), tile)
    return tile


def unpack(tile, place):
    return jnp.sum(tile[:, 3 * place : 3 * place + 3], axis=1, keepdims=True)


def repeat(out_ref, block):
    for part in range(out_ref.shape[0]):
        out_ref[part] = block


def load_body(offsets_ref, design_ref, out_ref, sems):
    parts = offsets_ref.shape[0]
    width = design_ref.shape[1] // parts
    copies = []
    for part in range(parts):
        offset = pl.multiple_of(offsets_ref[part], width)
        copies.append(
            pltpu.make_async_copy(
                design_ref.at[:, pl.ds(offset, width)],
                out_ref.at[:, pl.ds(part * width, width)],
                sems.at[part],
            )
        )
    for copy in copies:
        copy.start()
    for copy in copies:
        copy.wait()


def design_part(design_ref, place, width):
    return design_ref[:, place * width : (place + 1) * width]


def rows_body(places, again, *refs):
    *field_refs, design_ref, base_ref, out_ref = refs
    samples = design_ref.shape[0]
    blocks = []
    for field_ref in field_refs:
        if len(field_ref.shape) == 2:
            blocks.append(field_ref[...])
        else:
            blocks.extend(field_ref[row] for row in range(field_ref.shape[0]))
    strengths, width = blocks[0].shape
    total = jnp.zeros((strengths, samples), jnp.float32)
    squares = jnp.zeros((strengths, width), jnp.float32)
    products = jnp.zeros((strengths, width), jnp.float32)
    for index, place in enumerate(places):
        total += lax.dot_general(
            blocks[index],
            design_part(design_ref, place, width),
            (((1,), (1,)), ((), ())),
            preferred_element_type=jnp.float32,
        )
        values = blocks[index].astype(jnp.float32)
        squares += values * values
        if again:
            products += values * blocks[len(places) + index].astype(jnp.float32)
    square = jnp.sum(squares, axis=1, keepdims=True)
    sums = [square, jnp.sum(products, axis=1, keepdims=True)] if again else [square]
    base = base_ref[...]
    if base.shape[1] > LANES:
        out_ref[:, :samples] = base[:, :samples] + total
        out_ref[:, samples:] = base[:, samples:] + tile_of(*sums)
    else:
        out_ref[:, :samples] = total
        out_ref[:, samples:] = base + tile_of(*sums)


def columns(values, design_ref, places, out_refs, scale=None):
    targets = []
    for out_ref in out_refs:
        if len(out_ref.shape) == 2:
            targets.append((out_ref, ...))
        else:
            targets.extend((out_ref, row) for row in range(out_ref.shape[0]))
    for place, (out_ref, row) in zip(places, targets):
        block = lax.dot_general(
            values,
            design_part(design_ref, place, out_ref.shape[-1]),
            (((1,), (0,)), ((), ())),
            preferred_element_type=jnp.float32,
        )
        if scale is not None:
            block = block * scale
        out_ref[row] = block.astype(out_ref.dtype)


def miss_body(scale, places, both_ref, other_ref, labels_ref, design_ref, hessian_ref, miss_ref, *out_refs):
    samples = design_ref.shape[0]
    logits = both_ref[:, :samples] + other_ref[:, :samples]
    probability = 1.0 / (1.0 + jnp.exp(-logits))
    hessian_ref[...] = probability * (1.0 - probability)
    miss_rows = (probability - labels_ref[...].astype(jnp.float32)).astype(jnp.bfloat16)
    miss_ref[...] = miss_rows
    columns(miss_rows, design_ref, places, out_refs, scale)


def more_body(scale, places, values_ref, design_ref, *out_refs):
    columns(values_ref[...], design_ref, places, out_refs, scale)


def tile_of(*columns_in):
    rows = columns_in[0].shape[0]
    lane = lax.broadcasted_iota(jnp.int32, (rows, LANES), 1)
    tile = jnp.zeros((rows, LANES), jnp.float32)
    for place, column in enumerate(columns_in):
        tile = jnp.where(lane == place, column, tile)
    return tile


def dot_of(first, second):
    return jnp.sum(first * second, axis=1, keepdims=True)


def ratios_of(lam_ref, values_ref):
    lam = lam_ref[:, :1]
    values = values_ref[...]
    smallest = jnp.min(values, axis=1, keepdims=True)
    return (smallest + lam) / (values + lam) - 1.0


def gradient_body(summed_ref, weights_ref, lam_ref, sketch_ref, residual_ref, payload_ref):
    residual = -(summed_ref[...] + lam_ref[:, :1] * weights_ref[...])
    residual_ref[...] = residual
    repeat(payload_ref, exact_dot(residual, sketch_ref[...], 0).astype(jnp.bfloat16))


def first_body(
    summed_ref, other_ref, lam_ref, values_ref, sketch_ref, residual_ref,
    direction_ref, projected_ref, half_ref,
):
    projected = summed_ref[...] + other_ref[...]
    projected_ref[...] = projected
    scaled = ratios_of(lam_ref, values_ref) * projected
    direction = residual_ref[...] + exact_dot(scaled, sketch_ref[...], 1)
    direction_ref[...] = direction
    half_ref[...] = direction.astype(jnp.bfloat16)


def image_of(image_rows, hessian_ref):
    return (hessian_ref[...] * image_rows).astype(jnp.bfloat16)


def image_body(
    places, both_ref, other_ref, hessian_ref, design_ref, rows_ref, image_ref, scalars_ref, *out_refs
):
    samples = hessian_ref.shape[1]
    both = both_ref[...] + other_ref[...]
    image_rows = both[:, :samples]
    rows_ref[...] = image_rows
    image = image_of(image_rows, hessian_ref)
    image_ref[...] = image
    scalars_ref[...] = tile_of(
        both[:, samples : samples + 1], dot_of(image.astype(jnp.float32), image_rows)
    )
    columns(image, design_ref, places, out_refs)


def fold_body(own_ref, *refs):
    count = own_ref.shape[0]
    received_refs, target_refs = refs[:-count], refs[-count:]
    for row, target_ref in enumerate(target_refs):
        total = own_ref[row]
        for received_ref in received_refs:
            total += received_ref[row].astype(jnp.float32)
        target_ref[...] = total.astype(target_ref.dtype)


def image_project_body(count, own_ref, *refs):
    received_refs = refs[:count]
    scalars_ref, lam_ref, direction_ref, residual_ref, sketch_ref, applied_ref, payload_ref = refs[count:]
    rank = sketch_ref.shape[1]
    summed = own_ref[...]
    for received_ref in received_refs:
        summed += received_ref[...].astype(jnp.float32)
    applied = summed + lam_ref[:, :1] * direction_ref[...]
    applied_ref[...] = applied
    projected = exact_dot(applied, sketch_ref[...], 0).astype(jnp.bfloat16)
    residual = residual_ref[...]
    packed = pack(scalars_ref[:, 1:2], dot_of(residual, residual)).astype(jnp.bfloat16)
    for part in range(payload_ref.shape[0]):
        payload_ref[part, :, :rank] = projected
        payload_ref[part, :, rank:] = packed


def second_body(
    summed_ref, other_ref, lam_ref, values_ref, sketch_ref, scalars_ref, projected_ref,
    weights_ref, direction_ref, residual_ref, applied_ref,
    precond_ref, update_ref, known_ref, extra_ref, half_ref,
):
    rank = sketch_ref.shape[1]
    lam = lam_ref[:, :1]
    ratios = ratios_of(lam_ref, values_ref)
    projected = projected_ref[...]
    square = unpack(summed_ref[:, rank:] + other_ref[:, rank:], 1)
    energy = unpack(summed_ref[:, rank:], 0)
    res_dot = square + dot_of(ratios * projected, projected)
    step_size = res_dot / (energy + lam * scalars_ref[:, :1])
    residual = residual_ref[...] - step_size * applied_ref[...]
    projected = projected - step_size * (summed_ref[:, :rank] + other_ref[:, :rank])
    scaled = ratios * projected
    precond_res = residual + exact_dot(scaled, sketch_ref[...], 1)
    precond_ref[...] = precond_res
    half_ref[...] = precond_res.astype(jnp.bfloat16)
    update_ref[...] = weights_ref[...] + step_size * direction_ref[...]
    known_ref[...] = tile_of(res_dot, dot_of(scaled, projected), energy, scalars_ref[:, :1])
    zero = jnp.zeros_like(square)
    extra_ref[...] = tile_of(zero, zero, dot_of(residual, residual))


def energy_body(both_ref, other_ref, hessian_ref, rows_ref, squares_ref, payload_ref):
    samples = hessian_ref.shape[1]
    both = both_ref[...] + other_ref[...]
    squares_ref[...] = both[:, samples:]
    image_rows = both[:, :samples]
    image = image_of(image_rows, hessian_ref).astype(jnp.float32)
    sums = [dot_of(image, image_rows), dot_of(image, rows_ref[...]), both[:, samples + 2 : samples + 3]]
    lane = lax.broadcasted_iota(jnp.int32, (SUBLANES, LANES), 1)
    tile = jnp.zeros((SUBLANES, LANES), jnp.float32)
    for group in range(both.shape[0] // SUBLANES):
        for place, column in enumerate(sums):
            piece = column[group * SUBLANES : (group + 1) * SUBLANES]
            tile = jnp.where(lane == len(sums) * group + place, piece, tile)
    repeat(payload_ref, tile)


def finish_body(
    received_ref, squares_ref, known_ref, lam_ref, precond_ref, direction_ref, update_ref, out_ref
):
    tile = received_ref[0]
    for part in range(1, received_ref.shape[0]):
        tile += received_ref[part]
    groups = direction_ref.shape[0] // SUBLANES

    def total(place):
        lanes = [3 * group + place for group in range(groups)]
        return jnp.concatenate([tile[:, lane : lane + 1] for lane in lanes], axis=0)

    old_dot, part, old_energy, old_square = (known_ref[:, lane : lane + 1] for lane in range(4))
    res_dot = total(2) + part
    beta = res_dot / old_dot
    energy = total(0) + beta * (2.0 * total(1) + beta * old_energy)
    square = squares_ref[:, :1] + beta * (2.0 * squares_ref[:, 1:2] + beta * old_square)
    step_size = res_dot / (energy + lam_ref[:, :1] * square)
    direction = precond_ref[...] + beta * direction_ref[...]
    out_ref[...] = update_ref[...] + step_size * direction


VMEM = pl.BlockSpec(memory_space=pltpu.VMEM)


def call(body, shapes, *operands):
    return pl.pallas_call(
        body,
        out_shape=[jax.ShapeDtypeStruct(shape, dtype) for shape, dtype in shapes],
        in_specs=[VMEM] * len(operands),
        out_specs=[VMEM] * len(shapes),
        compiler_params=pltpu.CompilerParams(vmem_limit_bytes=8 << 20),
    )(*operands)


def load(design, offsets):
    return pl.pallas_call(
        load_body,
        out_shape=pltpu.VMEM(design.shape, design.dtype),
        in_specs=[pl.BlockSpec(memory_space=pltpu.SMEM), pl.BlockSpec(memory_space=pltpu.HBM)],
        out_specs=VMEM,
        scratch_shapes=[pltpu.SemaphoreType.DMA((offsets.shape[0],))],
        compiler_params=pltpu.CompilerParams(vmem_limit_bytes=1 << 20),
        name="load",
    )(offsets, design)


def make_shards(samp, feat):
    near = min(samp, 4)
    far = samp // near
    near_order = list(range(1, near))
    far_order = sorted(range(1, far), key=lambda distance: (distance * 2) % (far + 1))

    def swap(values, distance):
        return lax.ppermute(values, "samp", [(i, i ^ distance) for i in range(samp)])

    def swap_far(values):
        received = []
        for value, distance in zip(values, far_order):
            received.append(swap(value, near * distance))
        return received

    def swap_near(values):
        received = []
        for value, distance in zip(values, near_order):
            received.append(swap(value, distance))
        return received

    def gather(block):
        column = jnp.stack([block] + swap_far([block] * len(far_order)))
        return [column] + swap_near([column] * len(near_order))

    def exchange(blocks):
        return lax.all_to_all(blocks, "samp", 0, 0)

    def feat_parts(values):
        if feat == 2:
            return values, lax.ppermute(values, "feat", [(0, 1), (1, 0)])
        return lax.psum(values, "feat"), jnp.zeros_like(values)

    def shards(design_matrix, labels, weights, lambdas, sketch, sketch_values):
        strengths, width = weights.shape
        samples = design_matrix.shape[0]
        rank = sketch.shape[1]
        single, half = jnp.float32, jnp.bfloat16
        field = ((strengths, width), single)
        scalars = ((strengths, LANES), single)
        spread = ((strengths, width), half)
        payload = ((samp, strengths, rank), half)
        wide_payload = ((samp, strengths, rank + LANES), half)
        scale = 2.0 ** math.floor(math.log2(HALF_RANGE / (samples * near * LARGEST)))
        lam = jnp.broadcast_to(lambdas[:, None], (strengths, LANES))
        labels = labels[None, :]
        values = sketch_values[None, :]
        places = [k * near + j for j in [0] + near_order for k in [0] + far_order]
        places = jnp.bitwise_xor(lax.axis_index("samp"), jnp.array(places, jnp.int32))
        if width % LANES == 0:
            design = load(design_matrix, places * width)
        else:
            design = design_matrix.reshape(samples, samp, width)
            design = jnp.take(design, places, axis=1).reshape(design_matrix.shape)

        column_places = list(range(far))
        plane_places = list(range(far, samp))

        def apply_rows(fields, earlier, base):
            both = base
            for part in [0] + list(range(1, near))[::-1]:
                places = list(range(part * far, (part + 1) * far))
                old = earlier[part : part + 1]
                both = call(
                    lambda *refs: rows_body(places, len(old) > 0, *refs),
                    [((strengths, samples + LANES), single)], fields[part], *old, design, both,
                )[0]
            return feat_parts(both)

        def reduced(blocks):
            return feat_parts(jnp.sum(exchange(blocks).astype(single), axis=0))

        nothing = jnp.zeros((strengths, LANES), single)
        start = lax.optimization_barrier(weights.astype(half))
        sample_field = (strengths, samples)
        column = (far, strengths, width)
        hessian_diag, miss_rows, *outs = call(
            lambda *refs: miss_body(scale, plane_places, *refs),
            [(sample_field, single), (sample_field, half)] + [(column, single)] * (near - 1),
            *apply_rows(gather(start), [], nothing), labels, design,
        )
        folded = call(
            lambda *refs: more_body(scale, column_places, *refs),
            [(column, single)], miss_rows, design,
        )[0]
        for received in swap_near([out.astype(jnp.float16) for out in outs]):
            folded = folded + received.astype(single)
        summed = folded[0]
        for received in swap_far([folded[k].astype(jnp.float16) for k in range(1, far)]):
            summed = summed + received.astype(single)
        residual, blocks = call(
            gradient_body, [field, payload], summed * (1.0 / scale), weights, lam, sketch
        )
        direction, projected, block = call(
            first_body, [field, ((strengths, rank), single), spread],
            *reduced(blocks), lam, values, sketch, residual,
        )
        whole = gather(block)
        image_rows, image, known, *outs = call(
            lambda *refs: image_body(plane_places, *refs),
            [(sample_field, single), (sample_field, half), scalars] + [(column, half)] * (near - 1),
            *apply_rows(whole, [], nothing), hessian_diag, design,
        )
        own = call(
            lambda *refs: more_body(None, column_places, *refs),
            [(column, single)], image, design,
        )[0]
        kept, *sent = call(fold_body, [field] + [spread] * (far - 1), own, *swap_near(outs))
        applied, blocks = call(
            lambda *refs: image_project_body(far - 1, *refs), [field, wide_payload],
            kept, *swap_far(sent), known, lam, direction, residual, sketch,
        )
        precond_res, update, known, extra, block = call(
            second_body, [field, field, scalars, scalars, spread],
            *reduced(blocks), lam, values, sketch, known, projected,
            weights, direction, residual, applied,
        )
        squares, blocks = call(
            energy_body, [scalars, ((samp, SUBLANES, LANES), single)],
            *apply_rows(gather(block), whole, extra), hessian_diag, image_rows,
        )
        return call(
            finish_body, [field],
            exchange(blocks), squares, known, lam, precond_res, direction, update,
        )[0]

    return shards


def solution(mesh):
    return jax.shard_map(
        make_shards(mesh.shape["samp"], mesh.shape["feat"]),
        mesh=mesh,
        in_specs=(
            P("samp", "feat"),
            P("samp"),
            P(None, ("feat", "samp")),
            P(),
            P(("feat", "samp"), None),
            P(),
        ),
        out_specs=P(None, ("feat", "samp")),
        check_vma=False,
    )
```

```python
import math

import jax
import jax.numpy as jnp
from jax import lax
from jax.experimental import pallas as pl
from jax.experimental.pallas import tpu as pltpu
from jax.sharding import PartitionSpec as P


LANES = 128
SUBLANES = 8
LARGEST = 0.09375
HALF_RANGE = 60000.0


def split(values):
    high = values.astype(jnp.bfloat16)
    rest = values - high.astype(jnp.float32)
    middle = rest.astype(jnp.bfloat16)
    low = (rest - middle.astype(jnp.float32)).astype(jnp.bfloat16)
    return high, middle, low


def exact_dot(values, other, contract):
    rows = values.shape[0]
    product = lax.dot_general(
        jnp.concatenate([part.astype(jnp.float32) for part in split(values)], axis=0).astype(jnp.bfloat16),
        other,
        (((1,), (contract,)), ((), ())),
        preferred_element_type=jnp.float32,
    )
    return product[:rows] + product[rows : 2 * rows] + product[2 * rows :]


def pack(*columns_in):
    rows = columns_in[0].shape[0]
    lane = lax.broadcasted_iota(jnp.int32, (rows, LANES), 1)
    tile = jnp.zeros((rows, LANES), jnp.float32)
    for place, column in enumerate(columns_in):
        for index, part in enumerate(split(column)):
            tile = jnp.where(lane == 3 * place + index, part.astype(jnp.float32), tile)
    return tile


def unpack(tile, place):
    return jnp.sum(tile[:, 3 * place : 3 * place + 3], axis=1, keepdims=True)


def repeat(out_ref, block):
    for part in range(out_ref.shape[0]):
        out_ref[part] = block


def load_body(order, *refs):
    *design_refs, out_ref, sems = refs
    mine = lax.axis_index("samp")
    width = design_refs[0].shape[1] // len(order)
    copies = []
    for part, place in enumerate(order):
        offset = pl.multiple_of(jnp.bitwise_xor(mine, place) * width, width)
        for index, design_ref in enumerate(design_refs):
            slot = part * len(design_refs) + index
            copies.append(
                pltpu.make_async_copy(
                    design_ref.at[:, pl.ds(offset, width)],
                    out_ref.at[:, pl.ds(slot * width, width)],
                    sems.at[slot],
                )
            )
    for copy in copies:
        copy.start()
    for copy in copies:
        copy.wait()


def design_part(design_ref, place, width):
    return design_ref[:, place * width : (place + 1) * width]


def rows_body(places, again, *refs):
    *field_refs, design_ref, base_ref, out_ref = refs
    samples = design_ref.shape[0]
    blocks = []
    for field_ref in field_refs:
        if len(field_ref.shape) == 2:
            blocks.append(field_ref[...])
        else:
            blocks.extend(field_ref[row] for row in range(field_ref.shape[0]))
    strengths, width = blocks[0].shape
    total = jnp.zeros((strengths, samples), jnp.float32)
    squares = jnp.zeros((strengths, width), jnp.float32)
    products = jnp.zeros((strengths, width), jnp.float32)
    for index, place in enumerate(places):
        total += lax.dot_general(
            blocks[index],
            design_part(design_ref, place, width),
            (((1,), (1,)), ((), ())),
            preferred_element_type=jnp.float32,
        )
        values = blocks[index].astype(jnp.float32)
        squares += values * values
        if again:
            products += values * blocks[len(places) + index].astype(jnp.float32)
    square = jnp.sum(squares, axis=1, keepdims=True)
    sums = [square, jnp.sum(products, axis=1, keepdims=True)] if again else [square]
    base = base_ref[...]
    if base.shape[1] > LANES:
        out_ref[:, :samples] = base[:, :samples] + total
        out_ref[:, samples:] = base[:, samples:] + tile_of(*sums)
    else:
        out_ref[:, :samples] = total
        out_ref[:, samples:] = base + tile_of(*sums)


def columns(values, design_ref, places, out_refs, scale=None):
    targets = []
    for out_ref in out_refs:
        if len(out_ref.shape) == 2:
            targets.append((out_ref, ...))
        else:
            targets.extend((out_ref, row) for row in range(out_ref.shape[0]))
    for place, (out_ref, row) in zip(places, targets):
        block = lax.dot_general(
            values,
            design_part(design_ref, place, out_ref.shape[-1]),
            (((1,), (0,)), ((), ())),
            preferred_element_type=jnp.float32,
        )
        if scale is not None:
            block = block * scale
        out_ref[row] = block.astype(out_ref.dtype)


def miss_body(scale, places, both_ref, other_ref, labels_ref, design_ref, hessian_ref, miss_ref, *out_refs):
    samples = design_ref.shape[0]
    logits = both_ref[:, :samples] + other_ref[:, :samples]
    probability = 1.0 / (1.0 + jnp.exp(-logits))
    hessian_ref[...] = probability * (1.0 - probability)
    miss_rows = (probability - labels_ref[...].astype(jnp.float32)).astype(jnp.bfloat16)
    miss_ref[...] = miss_rows
    columns(miss_rows, design_ref, places, out_refs, scale)


def more_body(scale, places, values_ref, design_ref, *out_refs):
    columns(values_ref[...], design_ref, places, out_refs, scale)


def tile_of(*columns_in):
    rows = columns_in[0].shape[0]
    lane = lax.broadcasted_iota(jnp.int32, (rows, LANES), 1)
    tile = jnp.zeros((rows, LANES), jnp.float32)
    for place, column in enumerate(columns_in):
        tile = jnp.where(lane == place, column, tile)
    return tile


def dot_of(first, second):
    return jnp.sum(first * second, axis=1, keepdims=True)


def ratios_of(lam_ref, values_ref):
    lam = lam_ref[:, :1]
    values = values_ref[...]
    smallest = jnp.min(values, axis=1, keepdims=True)
    return (smallest + lam) / (values + lam) - 1.0


def gradient_body(summed_ref, weights_ref, lam_ref, sketch_ref, residual_ref, payload_ref):
    residual = -(summed_ref[...] + lam_ref[:, :1] * weights_ref[...])
    residual_ref[...] = residual
    repeat(payload_ref, exact_dot(residual, sketch_ref[...], 0).astype(jnp.bfloat16))


def first_body(
    summed_ref, other_ref, lam_ref, values_ref, sketch_ref, residual_ref,
    direction_ref, projected_ref, half_ref,
):
    projected = summed_ref[...] + other_ref[...]
    projected_ref[...] = projected
    scaled = ratios_of(lam_ref, values_ref) * projected
    direction = residual_ref[...] + exact_dot(scaled, sketch_ref[...], 1)
    direction_ref[...] = direction
    half_ref[...] = direction.astype(jnp.bfloat16)


def image_of(image_rows, hessian_ref):
    return (hessian_ref[...] * image_rows).astype(jnp.bfloat16)


def image_body(
    places, both_ref, other_ref, hessian_ref, design_ref, rows_ref, image_ref, scalars_ref, *out_refs
):
    samples = hessian_ref.shape[1]
    both = both_ref[...] + other_ref[...]
    image_rows = both[:, :samples]
    rows_ref[...] = image_rows
    image = image_of(image_rows, hessian_ref)
    image_ref[...] = image
    scalars_ref[...] = tile_of(
        both[:, samples : samples + 1], dot_of(image.astype(jnp.float32), image_rows)
    )
    columns(image, design_ref, places, out_refs)


def fold_body(own_ref, *refs):
    count = own_ref.shape[0]
    received_refs, target_refs = refs[:-count], refs[-count:]
    for row, target_ref in enumerate(target_refs):
        total = own_ref[row]
        for received_ref in received_refs:
            total += received_ref[row].astype(jnp.float32)
        target_ref[...] = total.astype(target_ref.dtype)


def image_project_body(count, own_ref, *refs):
    received_refs = refs[:count]
    scalars_ref, lam_ref, direction_ref, residual_ref, sketch_ref, applied_ref, payload_ref = refs[count:]
    rank = sketch_ref.shape[1]
    summed = own_ref[...]
    for received_ref in received_refs:
        summed += received_ref[...].astype(jnp.float32)
    applied = summed + lam_ref[:, :1] * direction_ref[...]
    applied_ref[...] = applied
    projected = exact_dot(applied, sketch_ref[...], 0).astype(jnp.bfloat16)
    residual = residual_ref[...]
    packed = pack(scalars_ref[:, 1:2], dot_of(residual, residual)).astype(jnp.bfloat16)
    for part in range(payload_ref.shape[0]):
        payload_ref[part, :, :rank] = projected
        payload_ref[part, :, rank:] = packed


def second_body(
    summed_ref, other_ref, lam_ref, values_ref, sketch_ref, scalars_ref, projected_ref,
    weights_ref, direction_ref, residual_ref, applied_ref,
    precond_ref, update_ref, known_ref, extra_ref, half_ref,
):
    rank = sketch_ref.shape[1]
    lam = lam_ref[:, :1]
    ratios = ratios_of(lam_ref, values_ref)
    projected = projected_ref[...]
    square = unpack(summed_ref[:, rank:] + other_ref[:, rank:], 1)
    energy = unpack(summed_ref[:, rank:], 0)
    res_dot = square + dot_of(ratios * projected, projected)
    step_size = res_dot / (energy + lam * scalars_ref[:, :1])
    residual = residual_ref[...] - step_size * applied_ref[...]
    projected = projected - step_size * (summed_ref[:, :rank] + other_ref[:, :rank])
    scaled = ratios * projected
    precond_res = residual + exact_dot(scaled, sketch_ref[...], 1)
    precond_ref[...] = precond_res
    half_ref[...] = precond_res.astype(jnp.bfloat16)
    update_ref[...] = weights_ref[...] + step_size * direction_ref[...]
    known_ref[...] = tile_of(res_dot, dot_of(scaled, projected), energy, scalars_ref[:, :1])
    zero = jnp.zeros_like(square)
    extra_ref[...] = tile_of(zero, zero, dot_of(residual, residual))


def energy_body(both_ref, other_ref, hessian_ref, rows_ref, squares_ref, payload_ref):
    samples = hessian_ref.shape[1]
    both = both_ref[...] + other_ref[...]
    squares_ref[...] = both[:, samples:]
    image_rows = both[:, :samples]
    image = image_of(image_rows, hessian_ref).astype(jnp.float32)
    sums = [dot_of(image, image_rows), dot_of(image, rows_ref[...]), both[:, samples + 2 : samples + 3]]
    lane = lax.broadcasted_iota(jnp.int32, (SUBLANES, LANES), 1)
    tile = jnp.zeros((SUBLANES, LANES), jnp.float32)
    for group in range(both.shape[0] // SUBLANES):
        for place, column in enumerate(sums):
            piece = column[group * SUBLANES : (group + 1) * SUBLANES]
            tile = jnp.where(lane == len(sums) * group + place, piece, tile)
    repeat(payload_ref, tile)


def finish_body(
    received_ref, squares_ref, known_ref, lam_ref, precond_ref, direction_ref, update_ref, out_ref
):
    tile = received_ref[0]
    for part in range(1, received_ref.shape[0]):
        tile += received_ref[part]
    groups = direction_ref.shape[0] // SUBLANES

    def total(place):
        lanes = [3 * group + place for group in range(groups)]
        return jnp.concatenate([tile[:, lane : lane + 1] for lane in lanes], axis=0)

    old_dot, part, old_energy, old_square = (known_ref[:, lane : lane + 1] for lane in range(4))
    res_dot = total(2) + part
    beta = res_dot / old_dot
    energy = total(0) + beta * (2.0 * total(1) + beta * old_energy)
    square = squares_ref[:, :1] + beta * (2.0 * squares_ref[:, 1:2] + beta * old_square)
    step_size = res_dot / (energy + lam_ref[:, :1] * square)
    direction = precond_ref[...] + beta * direction_ref[...]
    out_ref[...] = update_ref[...] + step_size * direction


VMEM = pl.BlockSpec(memory_space=pltpu.VMEM)


def call(body, shapes, *operands):
    return pl.pallas_call(
        body,
        out_shape=[jax.ShapeDtypeStruct(shape, dtype) for shape, dtype in shapes],
        in_specs=[VMEM] * len(operands),
        out_specs=[VMEM] * len(shapes),
        compiler_params=pltpu.CompilerParams(vmem_limit_bytes=24 << 20),
    )(*operands)


def load(designs, order):
    rows, block = designs[0].shape
    return pl.pallas_call(
        lambda *refs: load_body(order, *refs),
        out_shape=pltpu.VMEM((rows, block * len(designs)), designs[0].dtype),
        in_specs=[pl.BlockSpec(memory_space=pltpu.HBM)] * len(designs),
        out_specs=VMEM,
        scratch_shapes=[pltpu.SemaphoreType.DMA((len(order) * len(designs),))],
        compiler_params=pltpu.CompilerParams(vmem_limit_bytes=1 << 20),
        name="load",
    )(*designs)


def make_shards(samp, feat):
    near = min(samp, 4)
    far = samp // near
    near_order = list(range(1, near))
    far_order = sorted(range(1, far), key=lambda distance: (distance * 2) % (far + 1))

    def swap(values, distance):
        return lax.ppermute(values, "samp", [(i, i ^ distance) for i in range(samp)])

    def swap_far(values):
        received = []
        for value, distance in zip(values, far_order):
            received.append(swap(value, near * distance))
        return received

    def swap_near(values):
        received = []
        for value, distance in zip(values, near_order):
            received.append(swap(value, distance))
        return received

    def gather(block):
        column = jnp.stack([block] + swap_far([block] * len(far_order)))
        return [column] + swap_near([column] * len(near_order))

    def exchange(blocks):
        return lax.all_to_all(blocks, "samp", 0, 0)

    paired = feat == 2

    def feat_parts(values):
        if paired:
            return values, jnp.zeros_like(values)
        return lax.psum(values, "feat"), jnp.zeros_like(values)

    def partner(values):
        return lax.ppermute(values, "feat", [(0, 1), (1, 0)])

    def shards(design_matrix, labels, weights, lambdas, sketch, sketch_values):
        if not paired:
            return solve([design_matrix], labels, weights, lambdas, sketch, sketch_values)
        core = lax.axis_index("feat")
        count = weights.shape[0] // 2
        width = weights.shape[1]
        mine = lax.dynamic_slice_in_dim(weights, core * count, count, 0)
        theirs = partner(lax.dynamic_slice_in_dim(weights, (1 - core) * count, count, 0))
        result = solve(
            [design_matrix, partner(design_matrix)],
            labels,
            jnp.concatenate([mine, theirs], axis=1),
            lax.dynamic_slice_in_dim(lambdas, core * count, count, 0),
            jnp.concatenate([sketch, partner(sketch)], axis=0),
            sketch_values,
        )
        kept, other = result[:, :width], partner(result[:, width:])
        first = jnp.where(core == 0, kept, other)
        second = jnp.where(core == 0, other, kept)
        return jnp.concatenate([first, second], axis=0)

    def solve(designs, labels, weights, lambdas, sketch, sketch_values):
        strengths, width = weights.shape
        samples = designs[0].shape[0]
        rank = sketch.shape[1]
        single, half = jnp.float32, jnp.bfloat16
        field = ((strengths, width), single)
        scalars = ((strengths, LANES), single)
        spread = ((strengths, width), half)
        payload = ((samp, strengths, rank), half)
        wide_payload = ((samp, strengths, rank + LANES), half)
        scale = 2.0 ** math.floor(math.log2(HALF_RANGE / (samples * near * LARGEST)))
        lam = jnp.broadcast_to(lambdas[:, None], (strengths, LANES))
        labels = labels[None, :]
        values = sketch_values[None, :]
        places = [k * near + j for j in [0] + near_order for k in [0] + far_order]
        if width % LANES == 0:
            design = load(designs, places)
        else:
            places = jnp.bitwise_xor(lax.axis_index("samp"), jnp.array(places, jnp.int32))
            design = designs[0].reshape(samples, samp, width)
            design = jnp.take(design, places, axis=1).reshape(designs[0].shape)

        column_places = list(range(far))
        plane_places = list(range(far, samp))

        def apply_rows(fields, earlier, base):
            both = base
            for part in [0] + list(range(1, near))[::-1]:
                places = list(range(part * far, (part + 1) * far))
                old = earlier[part : part + 1]
                both = call(
                    lambda *refs: rows_body(places, len(old) > 0, *refs),
                    [((strengths, samples + LANES), single)], fields[part], *old, design, both,
                )[0]
            return feat_parts(both)

        def reduced(blocks):
            return feat_parts(jnp.sum(exchange(blocks).astype(single), axis=0))

        nothing = jnp.zeros((strengths, LANES), single)
        start = lax.optimization_barrier(weights.astype(half))
        sample_field = (strengths, samples)
        column = (far, strengths, width)
        hessian_diag, miss_rows, *outs = call(
            lambda *refs: miss_body(scale, plane_places, *refs),
            [(sample_field, single), (sample_field, half)] + [(column, single)] * (near - 1),
            *apply_rows(gather(start), [], nothing), labels, design,
        )
        folded = call(
            lambda *refs: more_body(scale, column_places, *refs),
            [(column, single)], miss_rows, design,
        )[0]
        for received in swap_near([out.astype(jnp.float16) for out in outs]):
            folded = folded + received.astype(single)
        summed = folded[0]
        for received in swap_far([folded[k].astype(jnp.float16) for k in range(1, far)]):
            summed = summed + received.astype(single)
        residual, blocks = call(
            gradient_body, [field, payload], summed * (1.0 / scale), weights, lam, sketch
        )
        direction, projected, block = call(
            first_body, [field, ((strengths, rank), single), spread],
            *reduced(blocks), lam, values, sketch, residual,
        )
        whole = gather(block)
        image_rows, image, known, *outs = call(
            lambda *refs: image_body(plane_places, *refs),
            [(sample_field, single), (sample_field, half), scalars] + [(column, half)] * (near - 1),
            *apply_rows(whole, [], nothing), hessian_diag, design,
        )
        own = call(
            lambda *refs: more_body(None, column_places, *refs),
            [(column, single)], image, design,
        )[0]
        kept, *sent = call(fold_body, [field] + [spread] * (far - 1), own, *swap_near(outs))
        applied, blocks = call(
            lambda *refs: image_project_body(far - 1, *refs), [field, wide_payload],
            kept, *swap_far(sent), known, lam, direction, residual, sketch,
        )
        precond_res, update, known, extra, block = call(
            second_body, [field, field, scalars, scalars, spread],
            *reduced(blocks), lam, values, sketch, known, projected,
            weights, direction, residual, applied,
        )
        squares, blocks = call(
            energy_body, [scalars, ((samp, SUBLANES, LANES), single)],
            *apply_rows(gather(block), whole, extra), hessian_diag, image_rows,
        )
        return call(
            finish_body, [field],
            exchange(blocks), squares, known, lam, precond_res, direction, update,
        )[0]

    return shards


def solution(mesh):
    return jax.shard_map(
        make_shards(mesh.shape["samp"], mesh.shape["feat"]),
        mesh=mesh,
        in_specs=(
            P("samp", "feat"),
            P("samp"),
            P(None, ("feat", "samp")),
            P(),
            P(("feat", "samp"), None),
            P(),
        ),
        out_specs=P(None, ("feat", "samp")),
        check_vma=False,
    )
```

```python
import math

import jax
import jax.numpy as jnp
from jax import lax
from jax.experimental import pallas as pl
from jax.experimental.pallas import tpu as pltpu
from jax.sharding import PartitionSpec as P


LANES = 128
SUBLANES = 8
LARGEST = 0.09375
HALF_RANGE = 60000.0


def split(values):
    high = values.astype(jnp.bfloat16)
    rest = values - high.astype(jnp.float32)
    middle = rest.astype(jnp.bfloat16)
    low = (rest - middle.astype(jnp.float32)).astype(jnp.bfloat16)
    return high, middle, low


def exact_dot(values, other, contract):
    rows = values.shape[0]
    product = lax.dot_general(
        jnp.concatenate([part.astype(jnp.float32) for part in split(values)], axis=0).astype(jnp.bfloat16),
        other,
        (((1,), (contract,)), ((), ())),
        preferred_element_type=jnp.float32,
    )
    return product[:rows] + product[rows : 2 * rows] + product[2 * rows :]


def pack(*columns_in):
    rows = columns_in[0].shape[0]
    lane = lax.broadcasted_iota(jnp.int32, (rows, LANES), 1)
    tile = jnp.zeros((rows, LANES), jnp.float32)
    for place, column in enumerate(columns_in):
        for index, part in enumerate(split(column)):
            tile = jnp.where(lane == 3 * place + index, part.astype(jnp.float32), tile)
    return tile


def unpack(tile, place):
    return jnp.sum(tile[:, 3 * place : 3 * place + 3], axis=1, keepdims=True)


def repeat(out_ref, block):
    for part in range(out_ref.shape[0]):
        out_ref[part] = block


def load_body(order, *refs):
    *design_refs, out_ref, sems = refs
    mine = lax.axis_index("samp")
    width = design_refs[0].shape[1] // len(order)
    copies = []
    for part, place in enumerate(order):
        offset = pl.multiple_of(jnp.bitwise_xor(mine, place) * width, width)
        for index, design_ref in enumerate(design_refs):
            slot = part * len(design_refs) + index
            copies.append(
                pltpu.make_async_copy(
                    design_ref.at[:, pl.ds(offset, width)],
                    out_ref.at[:, pl.ds(slot * width, width)],
                    sems.at[slot],
                )
            )
    for copy in copies:
        copy.start()
    for copy in copies:
        copy.wait()


def design_part(design_ref, place, width):
    return design_ref[:, place * width : (place + 1) * width]


def rows_body(places, again, *refs):
    *field_refs, design_ref, base_ref, out_ref = refs
    samples = design_ref.shape[0]
    blocks = []
    for field_ref in field_refs:
        if len(field_ref.shape) == 2:
            blocks.append(field_ref[...])
        else:
            blocks.extend(field_ref[row] for row in range(field_ref.shape[0]))
    strengths, width = blocks[0].shape
    total = jnp.zeros((strengths, samples), jnp.float32)
    squares = jnp.zeros((strengths, width), jnp.float32)
    products = jnp.zeros((strengths, width), jnp.float32)
    for index, place in enumerate(places):
        total += lax.dot_general(
            blocks[index],
            design_part(design_ref, place, width),
            (((1,), (1,)), ((), ())),
            preferred_element_type=jnp.float32,
        )
        values = blocks[index].astype(jnp.float32)
        squares += values * values
        if again:
            products += values * blocks[len(places) + index].astype(jnp.float32)
    square = jnp.sum(squares, axis=1, keepdims=True)
    sums = [square, jnp.sum(products, axis=1, keepdims=True)] if again else [square]
    base = base_ref[...]
    if base.shape[1] > LANES:
        out_ref[:, :samples] = base[:, :samples] + total
        out_ref[:, samples:] = base[:, samples:] + tile_of(*sums)
    else:
        out_ref[:, :samples] = total
        out_ref[:, samples:] = base + tile_of(*sums)


def columns(values, design_ref, places, out_refs, scale=None):
    targets = []
    for out_ref in out_refs:
        if len(out_ref.shape) == 2:
            targets.append((out_ref, ...))
        else:
            targets.extend((out_ref, row) for row in range(out_ref.shape[0]))
    for place, (out_ref, row) in zip(places, targets):
        block = lax.dot_general(
            values,
            design_part(design_ref, place, out_ref.shape[-1]),
            (((1,), (0,)), ((), ())),
            preferred_element_type=jnp.float32,
        )
        if scale is not None:
            block = block * scale
        out_ref[row] = block.astype(out_ref.dtype)


def miss_body(scale, places, both_ref, other_ref, labels_ref, design_ref, hessian_ref, miss_ref, *out_refs):
    samples = design_ref.shape[0]
    logits = both_ref[:, :samples] + other_ref[:, :samples]
    probability = 1.0 / (1.0 + jnp.exp(-logits))
    hessian_ref[...] = probability * (1.0 - probability)
    miss_rows = (probability - labels_ref[...].astype(jnp.float32)).astype(jnp.bfloat16)
    miss_ref[...] = miss_rows
    columns(miss_rows, design_ref, places, out_refs, scale)


def more_body(scale, places, values_ref, design_ref, *out_refs):
    columns(values_ref[...], design_ref, places, out_refs, scale)


def tile_of(*columns_in):
    rows = columns_in[0].shape[0]
    lane = lax.broadcasted_iota(jnp.int32, (rows, LANES), 1)
    tile = jnp.zeros((rows, LANES), jnp.float32)
    for place, column in enumerate(columns_in):
        tile = jnp.where(lane == place, column, tile)
    return tile


def dot_of(first, second):
    return jnp.sum(first * second, axis=1, keepdims=True)


def ratios_of(lam_ref, values_ref):
    lam = lam_ref[:, :1]
    values = values_ref[...]
    smallest = jnp.min(values, axis=1, keepdims=True)
    return (smallest + lam) / (values + lam) - 1.0


def gradient_body(
    summed_ref, weights_ref, lam_ref, values_ref, sketch_ref, residual_ref, payload_ref
):
    del values_ref
    residual = -(summed_ref[...] + lam_ref[:, :1] * weights_ref[...])
    residual_ref[...] = residual
    repeat(payload_ref, exact_dot(residual, sketch_ref[...], 0).astype(jnp.bfloat16))


def first_body(
    summed_ref, other_ref, lam_ref, values_ref, sketch_ref, residual_ref,
    direction_ref, projected_ref, half_ref,
):
    projected = summed_ref[...] + other_ref[...]
    projected_ref[...] = projected
    scaled = ratios_of(lam_ref, values_ref) * projected
    direction = residual_ref[...] + exact_dot(scaled, sketch_ref[...], 1)
    direction_ref[...] = direction
    half_ref[...] = direction.astype(jnp.bfloat16)


def image_of(image_rows, hessian_ref):
    return (hessian_ref[...] * image_rows).astype(jnp.bfloat16)


def image_body(
    places, both_ref, other_ref, hessian_ref, design_ref, rows_ref, image_ref, scalars_ref, *out_refs
):
    samples = hessian_ref.shape[1]
    both = both_ref[...] + other_ref[...]
    image_rows = both[:, :samples]
    rows_ref[...] = image_rows
    image = image_of(image_rows, hessian_ref)
    image_ref[...] = image
    scalars_ref[...] = tile_of(
        both[:, samples : samples + 1], dot_of(image.astype(jnp.float32), image_rows)
    )
    columns(image, design_ref, places, out_refs)


def fold_body(own_ref, *refs):
    count = own_ref.shape[0]
    received_refs, target_refs = refs[:-count], refs[-count:]
    for row, target_ref in enumerate(target_refs):
        total = own_ref[row]
        for received_ref in received_refs:
            total += received_ref[row].astype(jnp.float32)
        target_ref[...] = total.astype(target_ref.dtype)


def image_project_body(count, own_ref, *refs):
    received_refs = refs[:count]
    scalars_ref, lam_ref, direction_ref, residual_ref, sketch_ref, applied_ref, payload_ref = refs[count:]
    rank = sketch_ref.shape[1]
    summed = own_ref[...]
    for received_ref in received_refs:
        summed += received_ref[...].astype(jnp.float32)
    applied = summed + lam_ref[:, :1] * direction_ref[...]
    applied_ref[...] = applied
    projected = exact_dot(applied, sketch_ref[...], 0).astype(jnp.bfloat16)
    residual = residual_ref[...]
    packed = pack(scalars_ref[:, 1:2], dot_of(residual, residual)).astype(jnp.bfloat16)
    for part in range(payload_ref.shape[0]):
        payload_ref[part, :, :rank] = projected
        payload_ref[part, :, rank:] = packed


def second_body(
    summed_ref, other_ref, lam_ref, values_ref, sketch_ref, scalars_ref, projected_ref,
    weights_ref, direction_ref, residual_ref, applied_ref,
    precond_ref, update_ref, known_ref, extra_ref, half_ref,
):
    rank = sketch_ref.shape[1]
    lam = lam_ref[:, :1]
    ratios = ratios_of(lam_ref, values_ref)
    projected = projected_ref[...]
    square = unpack(summed_ref[:, rank:] + other_ref[:, rank:], 1)
    energy = unpack(summed_ref[:, rank:], 0)
    res_dot = square + dot_of(ratios * projected, projected)
    step_size = res_dot / (energy + lam * scalars_ref[:, :1])
    residual = residual_ref[...] - step_size * applied_ref[...]
    projected = projected - step_size * (summed_ref[:, :rank] + other_ref[:, :rank])
    scaled = ratios * projected
    precond_res = residual + exact_dot(scaled, sketch_ref[...], 1)
    precond_ref[...] = precond_res
    half_ref[...] = precond_res.astype(jnp.bfloat16)
    update_ref[...] = weights_ref[...] + step_size * direction_ref[...]
    known_ref[...] = tile_of(res_dot, dot_of(scaled, projected), energy, scalars_ref[:, :1])
    zero = jnp.zeros_like(square)
    extra_ref[...] = tile_of(zero, zero, dot_of(residual, residual))


def energy_body(both_ref, other_ref, hessian_ref, rows_ref, squares_ref, payload_ref):
    samples = hessian_ref.shape[1]
    both = both_ref[...] + other_ref[...]
    squares_ref[...] = both[:, samples:]
    image_rows = both[:, :samples]
    image = image_of(image_rows, hessian_ref).astype(jnp.float32)
    sums = [dot_of(image, image_rows), dot_of(image, rows_ref[...]), both[:, samples + 2 : samples + 3]]
    lane = lax.broadcasted_iota(jnp.int32, (SUBLANES, LANES), 1)
    tile = jnp.zeros((SUBLANES, LANES), jnp.float32)
    for group in range(both.shape[0] // SUBLANES):
        for place, column in enumerate(sums):
            piece = column[group * SUBLANES : (group + 1) * SUBLANES]
            tile = jnp.where(lane == len(sums) * group + place, piece, tile)
    repeat(payload_ref, tile)


def finish_body(
    received_ref, squares_ref, known_ref, lam_ref, precond_ref, direction_ref, update_ref, out_ref
):
    tile = received_ref[0]
    for part in range(1, received_ref.shape[0]):
        tile += received_ref[part]
    groups = direction_ref.shape[0] // SUBLANES

    def total(place):
        lanes = [3 * group + place for group in range(groups)]
        return jnp.concatenate([tile[:, lane : lane + 1] for lane in lanes], axis=0)

    old_dot, part, old_energy, old_square = (known_ref[:, lane : lane + 1] for lane in range(4))
    res_dot = total(2) + part
    beta = res_dot / old_dot
    energy = total(0) + beta * (2.0 * total(1) + beta * old_energy)
    square = squares_ref[:, :1] + beta * (2.0 * squares_ref[:, 1:2] + beta * old_square)
    step_size = res_dot / (energy + lam_ref[:, :1] * square)
    direction = precond_ref[...] + beta * direction_ref[...]
    out_ref[...] = update_ref[...] + step_size * direction


VMEM = pl.BlockSpec(memory_space=pltpu.VMEM)


def call(body, shapes, *operands):
    return pl.pallas_call(
        body,
        out_shape=[jax.ShapeDtypeStruct(shape, dtype) for shape, dtype in shapes],
        in_specs=[VMEM] * len(operands),
        out_specs=[VMEM] * len(shapes),
        compiler_params=pltpu.CompilerParams(vmem_limit_bytes=24 << 20),
    )(*operands)


def load(designs, order):
    rows, block = designs[0].shape
    return pl.pallas_call(
        lambda *refs: load_body(order, *refs),
        out_shape=pltpu.VMEM((rows, block * len(designs)), designs[0].dtype),
        in_specs=[pl.BlockSpec(memory_space=pltpu.HBM)] * len(designs),
        out_specs=VMEM,
        scratch_shapes=[pltpu.SemaphoreType.DMA((len(order) * len(designs),))],
        compiler_params=pltpu.CompilerParams(vmem_limit_bytes=1 << 20),
        name="load",
    )(*designs)


def make_shards(samp, feat):
    near = min(samp, 4)
    far = samp // near
    near_order = list(range(1, near))
    far_order = sorted(range(1, far), key=lambda distance: (distance * 2) % (far + 1))

    def swap(values, distance):
        return lax.ppermute(values, "samp", [(i, i ^ distance) for i in range(samp)])

    def swap_far(values):
        received = []
        for value, distance in zip(values, far_order):
            received.append(swap(value, near * distance))
        return received

    def swap_near(values):
        received = []
        for value, distance in zip(values, near_order):
            received.append(swap(value, distance))
        return received

    def gather(block):
        column = jnp.stack([block] + swap_far([block] * len(far_order)))
        return [column] + swap_near([column] * len(near_order))

    def exchange(blocks):
        return lax.all_to_all(blocks, "samp", 0, 0)

    paired = feat == 2

    def feat_parts(values):
        if paired:
            return values, jnp.zeros_like(values)
        return lax.psum(values, "feat"), jnp.zeros_like(values)

    def partner(values):
        return lax.ppermute(values, "feat", [(0, 1), (1, 0)])

    def shards(design_matrix, labels, weights, lambdas, sketch, sketch_values):
        if not paired:
            return solve([design_matrix], labels, weights, lambdas, sketch, sketch_values)
        core = lax.axis_index("feat")
        count = weights.shape[0] // 2
        width = weights.shape[1]
        mine = lax.dynamic_slice_in_dim(weights, core * count, count, 0)
        theirs = partner(lax.dynamic_slice_in_dim(weights, (1 - core) * count, count, 0))
        theirs, design_matrix, sketch = lax.optimization_barrier((theirs, design_matrix, sketch))
        result = solve(
            [design_matrix, partner(design_matrix)],
            labels,
            jnp.concatenate([mine, theirs], axis=1),
            lax.dynamic_slice_in_dim(lambdas, core * count, count, 0),
            jnp.concatenate([sketch, partner(sketch)], axis=0),
            sketch_values,
        )
        kept, other = result[:, :width], partner(result[:, width:])
        first = jnp.where(core == 0, kept, other)
        second = jnp.where(core == 0, other, kept)
        return jnp.concatenate([first, second], axis=0)

    def solve(designs, labels, weights, lambdas, sketch, sketch_values):
        strengths, width = weights.shape
        samples = designs[0].shape[0]
        rank = sketch.shape[1]
        single, half = jnp.float32, jnp.bfloat16
        field = ((strengths, width), single)
        scalars = ((strengths, LANES), single)
        spread = ((strengths, width), half)
        payload = ((samp, strengths, rank), half)
        wide_payload = ((samp, strengths, rank + LANES), half)
        scale = 2.0 ** math.floor(math.log2(HALF_RANGE / (samples * near * LARGEST)))
        lam = jnp.broadcast_to(lambdas[:, None], (strengths, LANES))
        labels = labels[None, :]
        values = sketch_values[None, :]
        places = [k * near + j for j in [0] + near_order for k in [0] + far_order]
        if width % LANES == 0:
            design = load(designs, places)
        else:
            places = jnp.bitwise_xor(lax.axis_index("samp"), jnp.array(places, jnp.int32))
            design = designs[0].reshape(samples, samp, width)
            design = jnp.take(design, places, axis=1).reshape(designs[0].shape)

        column_places = list(range(far))
        plane_places = list(range(far, samp))

        def apply_rows(fields, earlier, base):
            both = base
            for part in [0] + list(range(1, near))[::-1]:
                places = list(range(part * far, (part + 1) * far))
                old = earlier[part : part + 1]
                both = call(
                    lambda *refs: rows_body(places, len(old) > 0, *refs),
                    [((strengths, samples + LANES), single)], fields[part], *old, design, both,
                )[0]
            return feat_parts(both)

        def reduced(blocks):
            return feat_parts(jnp.sum(exchange(blocks).astype(single), axis=0))

        nothing = jnp.zeros((strengths, LANES), single)
        start = lax.optimization_barrier(weights.astype(half))
        sample_field = (strengths, samples)
        column = (far, strengths, width)
        hessian_diag, miss_rows, *outs = call(
            lambda *refs: miss_body(scale, plane_places, *refs),
            [(sample_field, single), (sample_field, half)] + [(column, single)] * (near - 1),
            *apply_rows(gather(start), [], nothing), labels, design,
        )
        folded = call(
            lambda *refs: more_body(scale, column_places, *refs),
            [(column, single)], miss_rows, design,
        )[0]
        for received in swap_near([out.astype(jnp.float16) for out in outs]):
            folded = folded + received.astype(single)
        summed = folded[0]
        for received in swap_far([folded[k].astype(jnp.float16) for k in range(1, far)]):
            summed = summed + received.astype(single)
        residual, blocks = call(
            gradient_body, [field, payload], summed * (1.0 / scale), weights, lam, values, sketch,
        )
        direction, projected, block = call(
            first_body, [field, ((strengths, rank), single), spread],
            *reduced(blocks), lam, values, sketch, residual,
        )
        whole = gather(block)
        image_rows, image, known, *outs = call(
            lambda *refs: image_body(plane_places, *refs),
            [(sample_field, single), (sample_field, half), scalars] + [(column, half)] * (near - 1),
            *apply_rows(whole, [], nothing), hessian_diag, design,
        )
        own = call(
            lambda *refs: more_body(None, column_places, *refs),
            [(column, single)], image, design,
        )[0]
        kept, *sent = call(fold_body, [field] + [spread] * (far - 1), own, *swap_near(outs))
        applied, blocks = call(
            lambda *refs: image_project_body(far - 1, *refs), [field, wide_payload],
            kept, *swap_far(sent), known, lam, direction, residual, sketch,
        )
        precond_res, update, known, extra, block = call(
            second_body, [field, field, scalars, scalars, spread],
            *reduced(blocks), lam, values, sketch, known, projected,
            weights, direction, residual, applied,
        )
        squares, blocks = call(
            energy_body, [scalars, ((samp, SUBLANES, LANES), single)],
            *apply_rows(gather(block), whole, extra), hessian_diag, image_rows,
        )
        return call(
            finish_body, [field],
            exchange(blocks), squares, known, lam, precond_res, direction, update,
        )[0]

    return shards


def solution(mesh):
    return jax.shard_map(
        make_shards(mesh.shape["samp"], mesh.shape["feat"]),
        mesh=mesh,
        in_specs=(
            P("samp", "feat"),
            P("samp"),
            P(None, ("feat", "samp")),
            P(),
            P(("feat", "samp"), None),
            P(),
        ),
        out_specs=P(None, ("feat", "samp")),
        check_vma=False,
    )
```
